32 devices in a mesh: dev: 32 (over z, y, x, core).
Axes of the slice: x: 2, y: 2, z: 4, core: 2. Of those that a mesh axis runs over, the one named last changes fastest.
Arguments:
- state_real: float32 [4194304], P('dev'), may hold values from -24 to 24, as said below
- state_imag: float32 [4194304], P('dev'), may hold values from -24 to 24, as said below
- subsystem: int32 [3], replicated, may hold values from 0 to 16, as said below
Outputs:
- rho_real: float32 [256, 256], P('dev')
- rho_imag: float32 [256, 256], P('dev')
The draws below stay inside these ranges and needn't reach their ends.
Inputs may be any that keep to these rules, and one draw needn't show every extreme that they name: `subsystem`: the 3 entries are distinct local bit positions in ascending order; the first is always 0 and the last always 17 - 1. `state_real`: real parts of amplitudes; their typical size changes between aligned blocks of 2**(11) local indices by up to a factor of 16. `state_imag`: imaginary parts of amplitudes, with the same block sizes as the real parts.
All inputs are finite; a program needn't handle non-finite values.
Results may differ from the reference program's by a relative error of at most 0.0001.
Values sent between devices are 32-bit elements; how exact they have to be, the bound alone decides.
A program may use at most 192 MiB of HBM per device.

```python
import jax
import jax.numpy as jnp
from jax import lax

LOCAL_QUBITS = 17
SUB_LOCAL = 3
AMPS_DEV = 131072
AMPS = 4194304
COMPLEMENT = 16384
SUB_DIM = 256
N_DEV = 32


def amplitude_envelope(key):
    block_total = AMPS // 2 ** (LOCAL_QUBITS - 6)
    levels = jax.random.uniform(jax.random.fold_in(key, 11), (block_total,), jnp.float32, -1.3862943611198906, 1.3862943611198906)
    return jnp.repeat(jnp.exp(levels), AMPS // block_total, total_repeat_length=AMPS)


def draw_noise(key, salt_value):
    noise_key = jax.random.fold_in(key, salt_value)
    return jnp.clip(jax.random.normal(noise_key, (AMPS,), jnp.float32), -6.0, 6.0)


def draw_state_real(key, part):
    return (amplitude_envelope(key) * draw_noise(key, 3)).astype(jnp.float32)


def draw_state_imag(key, part):
    return (amplitude_envelope(key) * draw_noise(key, 5)).astype(jnp.float32)


def draw_subsystem(key, part):
    middle = jax.random.randint(jax.random.fold_in(key, 17), (1,), 1, LOCAL_QUBITS - 1, jnp.int32)
    lowest = jnp.zeros((1,), jnp.int32)
    highest = jnp.full((1,), LOCAL_QUBITS - 1, jnp.int32)
    return jnp.concatenate([lowest, middle, highest]).astype(jnp.int32)


def setup_inputs(seed: int = 0) -> dict:
    arg_keys = jax.random.split(jax.random.key(seed), 4)
    state_real = draw_state_real(jax.random.fold_in(arg_keys[3], 71), 0)
    state_imag = draw_state_imag(jax.random.fold_in(arg_keys[3], 71), 0)
    subsystem = draw_subsystem(jax.random.fold_in(arg_keys[3], 71), 0)
    return dict(state_real=state_real, state_imag=state_imag, subsystem=subsystem)


def insert_bits(subsystem, count_sub, count_rest):
    picked = lax.broadcasted_iota(jnp.int32, (count_sub, count_rest), 0)
    source = lax.broadcasted_iota(jnp.int32, (count_sub, count_rest), 1)
    for sub_index in range(subsystem.shape[0]):
        bit_place = subsystem[sub_index].astype(jnp.int32)
        lower_bits = jnp.bitwise_and(source, jnp.left_shift(jnp.int32(1), bit_place) - jnp.int32(1))
        upper_bits = jnp.left_shift(jnp.right_shift(source, bit_place), bit_place + jnp.int32(1))
        chosen_bit = jnp.left_shift(jnp.bitwise_and(jnp.right_shift(picked, sub_index), jnp.int32(1)), bit_place)
        source = upper_bits + chosen_bit + lower_bits
    return source


def contract(left, right):
    return lax.dot_general(left, right, (((1,), (1,)), ((), ())), precision=lax.Precision.HIGHEST, preferred_element_type=jnp.float32)


def reference(state_real, state_imag, subsystem):
    source_map = insert_bits(subsystem, 2 ** SUB_LOCAL, COMPLEMENT)
    psi_real = state_real.reshape(N_DEV, AMPS_DEV)[:, source_map].reshape(SUB_DIM, COMPLEMENT)
    psi_imag = state_imag.reshape(N_DEV, AMPS_DEV)[:, source_map].reshape(SUB_DIM, COMPLEMENT)
    inverse_rest = 1.0 / COMPLEMENT
    rho_real = (contract(psi_real, psi_real) + contract(psi_imag, psi_imag)) * inverse_rest
    rho_imag = (contract(psi_imag, psi_real) - contract(psi_real, psi_imag)) * inverse_rest
    return rho_real, rho_imag
```

```python
import functools

import jax
import jax.numpy as jnp
from jax import lax
from jax.experimental import pallas as pl
from jax.experimental.pallas import tpu as pltpu
from jax.sharding import PartitionSpec as P

MESH = pl.DeviceIdType.MESH
PLANES = 4


def exchange_kernel(n, scale, sub_hbm, re_hbm, im_hbm, out_ref, sub_ref, state, mixed, send, recv,
                    high_ref, low_ref, part, turned_ref, chain, rows, load_sem, send_sem,
                    recv_sem, chain_sem, row_send, row_recv):
    me = lax.axis_index("dev")
    loads = [
        pltpu.make_async_copy(sub_hbm, sub_ref, load_sem.at[2]),
        pltpu.make_async_copy(re_hbm, state.at[0], load_sem.at[0]),
        pltpu.make_async_copy(im_hbm, state.at[1], load_sem.at[1]),
    ]
    for load in loads:
        load.start()
    barrier = pltpu.get_barrier_semaphore()

    def greet(k, carry):
        pl.semaphore_signal(
            barrier, inc=1, device_id=(jnp.bitwise_xor(me, n - k),), device_id_type=MESH
        )
        return carry

    lax.fori_loop(1, n, greet, 0)

    devs = n // PLANES
    chips = devs // 2
    owners = n // 2
    plane = me // devs
    chip = lax.rem(me, devs) // 2
    core = lax.rem(me, 2)
    low_half = plane < 2
    outer = (plane == 0) | (plane == PLANES - 1)
    inner = jnp.logical_not(outer)
    beside = jnp.bitwise_xor(plane, 1)
    far = jnp.where(low_half, 3, 0)
    across = jnp.where(low_half, 2, 1)

    vregs = state.shape[1]
    quarter = vregs // 4
    bits = vregs.bit_length() - 1
    width = vregs // owners
    full = 8 * n

    for load in loads:
        load.wait()

    lane = lax.broadcasted_iota(jnp.int32, (8, 128), 1)
    sub = lax.broadcasted_iota(jnp.int32, (8, 128), 0)

    mid = sub_ref[1]
    lane_step = jnp.int32(1)
    for b in range(1, 7):
        lane_step = jnp.where(mid == b, 2**b, lane_step)
    top = 10 + bits - 1
    in_lane = (mid < 7) | (mid == top - 1)
    stride = jnp.int32(vregs // 8)
    for b in range(10, top - 1):
        stride = jnp.where(mid == b, 2 ** (b - 10), stride)
    stride = jnp.where(mid == 7, vregs // 4, stride)
    stride = jnp.where(mid == 9, vregs // 2, stride)
    fixed = mid == 8
    lane_on = jnp.where(in_lane, lane_step, 0)
    lane_hit = jnp.bitwise_and(lane, lane_on) != 0
    lane_keep = lane_hit | (jnp.where(in_lane, 0, 1) != jnp.bitwise_and(lane, 0))
    sub_on = jnp.where(fixed, 0, 2)
    sub_hit = jnp.bitwise_and(sub, sub_on) != 0
    sub_keep = sub_hit | (jnp.where(fixed, 1, 0) != jnp.bitwise_and(sub, 0))

    high4 = sub >= 4
    odd_sub = jnp.bitwise_and(sub, 1) != 0
    odd_lane = jnp.bitwise_and(lane, 1) != 0

    def swap(a, b, hit, keep, step, axis):
        size = (8, 128)[axis]
        back = size - step
        return (
            jnp.where(hit, pltpu.roll(b, step, axis), a),
            jnp.where(keep, b, pltpu.roll(a, back, axis)),
        )

    def first_pass(v, carry):
        for c in range(2):
            x = [state[c, v + quarter * k] for k in range(4)]
            x[0], x[2] = swap(x[0], x[2], high4, high4, 4, 0)
            x[1], x[3] = swap(x[1], x[3], high4, high4, 4, 0)
            for k in (0, 2):
                a, b = swap(x[k], x[k + 1], odd_lane, odd_lane, 1, 1)
                x[k], x[k + 1] = swap(a, b, odd_sub, odd_sub, 1, 0)
            for k in range(4):
                mixed[c, v + quarter * k] = x[k]
        return carry

    lax.fori_loop(0, quarter, first_pass, 0, unroll=4)

    pairs = width // 2
    order = (
        jnp.where(outer, far, beside),
        jnp.where(outer, across, plane),
        jnp.where(outer, beside, far),
        jnp.where(outer, plane, across),
    )

    def target(k):
        at = k // chips
        zone = order[3]
        for i in (2, 1, 0):
            zone = jnp.where(at == i, order[i], zone)
        return zone, jnp.bitwise_xor(chip, chips - 1 - lax.rem(k, chips))

    def pack(k, carry):
        zone, where = target(k)
        owner = zone * chips + where
        for c in range(2):
            for p in range(pairs):
                u = owner * pairs + p
                low = jnp.bitwise_and(u, stride - 1)
                first = 2 * u - low
                a = mixed[c, first]
                b = mixed[c, first + stride]
                a, b = swap(a, b, lane_hit, lane_keep, lane_step, 1)
                a, b = swap(a, b, sub_hit, sub_keep, 2, 0)
                for w, value in enumerate((a, b)):
                    column = (c * width + 2 * p + w) * 128
                    send[owner, :, column : column + 128] = value
        return carry

    lax.fori_loop(0, chips, pack, 0)
    pl.semaphore_wait(barrier, n - 1)

    def send_chunk(k, carry):
        zone, where = target(k)
        owner = zone * chips + where
        device = zone * devs + 2 * where + 1

        @pl.when(device != me)
        def _():
            pltpu.make_async_remote_copy(
                src_ref=send.at[owner], dst_ref=recv.at[me], send_sem=send_sem,
                recv_sem=recv_sem.at[plane], device_id=(device,), device_id_type=MESH,
            ).start()

        @pl.when(device == me)
        def _():
            pltpu.make_async_copy(send.at[owner], recv.at[me], recv_sem.at[plane]).start()

        return carry

    def send_and_pack(k, carry):
        send_chunk(k, 0)
        pack(k + chips, 0)
        return carry

    lax.fori_loop(0, owners - chips, send_and_pack, 0)
    lax.fori_loop(owners - chips, owners, send_chunk, 0)

    depth = width * 128
    block = 8 * devs
    wide = max(block, 128)
    ratio = wide // block

    def split(x):
        high = x.astype(jnp.bfloat16)
        return high, (x - high.astype(jnp.float32)).astype(jnp.bfloat16)

    def dot(x, y):
        return lax.dot_general(x, y, (((1,), (1,)), ((), ())), preferred_element_type=jnp.float32)

    def stacked(x):
        return jnp.concatenate(
            [x, jnp.concatenate([x[:, depth:], -x[:, :depth]], axis=1)], axis=0
        )

    def arrival(s):
        second = jnp.where(outer, beside, far)
        third = jnp.where(outer, far, beside)
        return jnp.where(
            s == 0, plane, jnp.where(s == 1, second, jnp.where(s == 2, third, across))
        )

    def gram(s, carry):
        zone = arrival(s)
        mine = pl.ds(zone * devs, devs)
        lines = pl.ds(pl.multiple_of(zone * block, block), block)
        came = recv.at[mine]
        pltpu.make_async_copy(came, came, recv_sem.at[zone]).wait()
        high, low = split(recv[mine].reshape(block, 2 * depth))
        high_ref[lines] = high
        low_ref[lines] = low
        left_h = stacked(high)
        left_l = stacked(low)
        right_h = high_ref[...]
        result = dot(left_h, right_h) + (dot(left_h, low_ref[...]) + dot(left_l, right_h))
        column = pl.ds(pl.multiple_of(zone // ratio * wide, wide), wide)
        for c in range(2):
            value = result[c * block : (c + 1) * block]
            part[mine, :, c * full : (c + 1) * full] = value.reshape(devs, 8, full)
            if c == 1:
                value = -value
            if ratio > 1:
                slot = lax.rem(zone, ratio)
                value = jnp.concatenate(
                    [jnp.where(slot == r, value, 0.0) for r in range(ratio)], axis=0
                )
            turned_ref[c] = value.T.reshape(n, 8, wide)

        def mirror(e, carry):
            there = pl.ds(arrival(e) * devs, devs)
            for c in range(2):
                at = pl.ds(pl.multiple_of(c * full + zone // ratio * wide, wide), wide)
                part[there, :, at] = part[there, :, at] + turned_ref[c, there]
            return carry

        lax.fori_loop(0, s, mirror, 0)
        return carry

    def send_rows(zone, slot, ready):
        def one(k, carry):
            at = jnp.bitwise_xor(lax.rem(me, devs), devs - 1 - k)
            device = zone * devs + at
            ready(device)

            @pl.when(device != me)
            def _():
                pltpu.make_async_remote_copy(
                    src_ref=part.at[device], dst_ref=rows.at[slot, chip], send_sem=row_send,
                    recv_sem=row_recv.at[slot], device_id=(device,), device_id_type=MESH,
                ).start()

            @pl.when(device == me)
            def _():
                pltpu.make_async_copy(
                    part.at[device], rows.at[slot, chip], row_recv.at[slot]
                ).start()

            return carry

        lax.fori_loop(0, devs, one, 0)

    def add_chain(device):
        part[device] = part[device] + chain[device]

    @pl.when(core == 1)
    def _():
        high_ref[...] = jnp.zeros_like(high_ref)
        low_ref[...] = jnp.zeros_like(low_ref)
        lax.fori_loop(0, PLANES, gram, 0)

        @pl.when(outer)
        def _():
            for i, zone in enumerate((far, across, beside)):
                mine = pl.ds(zone * devs, devs)
                pltpu.make_async_remote_copy(
                    src_ref=part.at[mine], dst_ref=chain.at[mine], send_sem=row_send,
                    recv_sem=chain_sem.at[i], device_id=(beside * devs + 2 * chip + 1,),
                    device_id_type=MESH,
                ).start()
            send_rows(plane, 0, lambda device: None)

        @pl.when(inner)
        def _():
            send_rows(beside, 1, lambda device: None)
            for i, (zone, slot) in enumerate(((far, 2), (across, 2), (plane, 0))):
                came = chain.at[pl.ds(zone * devs, devs)]
                pltpu.make_async_copy(came, came, chain_sem.at[i]).wait()
                send_rows(zone, slot, add_chain)

    def gathered(slot):
        pltpu.make_async_copy(rows.at[slot], rows.at[slot], row_recv.at[slot]).wait()
        total = rows[slot, 0]
        for k in range(1, chips):
            total = total + rows[slot, k]
        return total

    out_ref[...] = gathered(0)

    @pl.when(outer)
    def _():
        out_ref[...] = out_ref[...] + gathered(1)

    out_ref[...] = (out_ref[...] + gathered(2)) * scale

    rest = send.at[pl.ds(0, owners - 1)]
    pltpu.make_async_copy(rest, rest, send_sem).wait()

    @pl.when(core == 0)
    def _():
        pltpu.make_async_copy(send.at[0], send.at[0], send_sem).wait()

    @pl.when(core == 1)
    def _():
        sent = part.at[pl.ds(0, n - 1)]
        pltpu.make_async_copy(sent, sent, row_send).wait()


def local(n, state_real, state_imag, subsystem):
    amps = state_real.shape[0]
    vregs = amps // 1024
    owners = n // 2
    width = vregs // owners
    full = 8 * n
    devs = n // PLANES
    wide = max(8 * devs, 128)
    chunk = (8, 2 * width * 128)
    out = pl.pallas_call(
        functools.partial(exchange_kernel, n, 8.0 / amps),
        out_shape=jax.ShapeDtypeStruct((8, 2 * full), jnp.float32),
        in_specs=[
            pl.BlockSpec(memory_space=pl.ANY),
            pl.BlockSpec(memory_space=pl.ANY),
            pl.BlockSpec(memory_space=pl.ANY),
        ],
        out_specs=pl.BlockSpec(memory_space=pltpu.VMEM),
        scratch_shapes=[
            pltpu.SMEM((3,), jnp.int32),
            pltpu.VMEM((2, vregs, 8, 128), jnp.float32),
            pltpu.VMEM((2, vregs, 8, 128), jnp.float32),
            pltpu.VMEM((owners,) + chunk, jnp.float32),
            pltpu.VMEM((n,) + chunk, jnp.float32),
            pltpu.VMEM((full, chunk[1]), jnp.bfloat16),
            pltpu.VMEM((full, chunk[1]), jnp.bfloat16),
            pltpu.VMEM((n, 8, 2 * full), jnp.float32),
            pltpu.VMEM((2, n, 8, wide), jnp.float32),
            pltpu.VMEM((n, 8, 2 * full), jnp.float32),
            pltpu.VMEM((3, devs // 2, 8, 2 * full), jnp.float32),
            pltpu.SemaphoreType.DMA((3,)),
            pltpu.SemaphoreType.DMA,
            pltpu.SemaphoreType.DMA((PLANES,)),
            pltpu.SemaphoreType.DMA((3,)),
            pltpu.SemaphoreType.DMA,
            pltpu.SemaphoreType.DMA((3,)),
        ],
        compiler_params=pltpu.CompilerParams(
            collective_id=0, has_side_effects=True, vmem_limit_bytes=56 * 2**20
        ),
    )(subsystem, state_real.reshape(vregs, 8, 128), state_imag.reshape(vregs, 8, 128))
    return out[:, :full], out[:, full:]


def solution(mesh):
    return jax.shard_map(
        functools.partial(local, mesh.shape["dev"]),
        mesh=mesh,
        in_specs=(P("dev"), P("dev"), P()),
        out_specs=(P("dev", None), P("dev", None)),
        check_vma=False,
    )
```

```python
import functools

import jax
import jax.numpy as jnp
from jax import lax
from jax.experimental import pallas as pl
from jax.experimental.pallas import tpu as pltpu
from jax.sharding import PartitionSpec as P

MESH = pl.DeviceIdType.MESH
PLANES = 4


def exchange_kernel(n, scale, sub_hbm, re_hbm, im_hbm, out_ref, sub_ref, state, mixed, send, recv,
                    high_ref, low_ref, part, turned_ref, chain, rows, load_sem, send_sem,
                    recv_sem, chain_sem, row_send, row_recv):
    me = lax.axis_index("dev")
    loads = [
        pltpu.make_async_copy(sub_hbm, sub_ref, load_sem.at[2]),
        pltpu.make_async_copy(re_hbm, state.at[0], load_sem.at[0]),
        pltpu.make_async_copy(im_hbm, state.at[1], load_sem.at[1]),
    ]
    for load in loads:
        load.start()
    barrier = pltpu.get_barrier_semaphore()

    def greet(k, carry):
        pl.semaphore_signal(
            barrier, inc=1, device_id=(jnp.bitwise_xor(me, n - k),), device_id_type=MESH
        )
        return carry

    lax.fori_loop(1, n, greet, 0)

    devs = n // PLANES
    chips = devs // 2
    owners = n // 2
    plane = me // devs
    chip = lax.rem(me, devs) // 2
    core = lax.rem(me, 2)
    low_half = plane < 2
    outer = (plane == 0) | (plane == PLANES - 1)
    inner = jnp.logical_not(outer)
    beside = jnp.bitwise_xor(plane, 1)
    far = jnp.where(low_half, 3, 0)
    across = jnp.where(low_half, 2, 1)

    vregs = state.shape[1]
    quarter = vregs // 4
    bits = vregs.bit_length() - 1
    width = vregs // owners
    full = 8 * n

    for load in loads:
        load.wait()

    lane = lax.broadcasted_iota(jnp.int32, (8, 128), 1)
    sub = lax.broadcasted_iota(jnp.int32, (8, 128), 0)

    mid = sub_ref[1]
    lane_step = jnp.int32(1)
    for b in range(1, 7):
        lane_step = jnp.where(mid == b, 2**b, lane_step)
    top = 10 + bits - 1
    in_lane = (mid < 7) | (mid == top - 1)
    stride = jnp.int32(vregs // 8)
    for b in range(10, top - 1):
        stride = jnp.where(mid == b, 2 ** (b - 10), stride)
    stride = jnp.where(mid == 7, vregs // 4, stride)
    stride = jnp.where(mid == 9, vregs // 2, stride)
    fixed = mid == 8
    lane_on = jnp.where(in_lane, lane_step, 0)
    lane_hit = jnp.bitwise_and(lane, lane_on) != 0
    lane_keep = lane_hit | (jnp.where(in_lane, 0, 1) != jnp.bitwise_and(lane, 0))
    sub_on = jnp.where(fixed, 0, 2)
    sub_hit = jnp.bitwise_and(sub, sub_on) != 0
    sub_keep = sub_hit | (jnp.where(fixed, 1, 0) != jnp.bitwise_and(sub, 0))

    high4 = sub >= 4
    odd_sub = jnp.bitwise_and(sub, 1) != 0
    odd_lane = jnp.bitwise_and(lane, 1) != 0

    def swap(a, b, hit, keep, step, axis):
        size = (8, 128)[axis]
        back = size - step
        return (
            jnp.where(hit, pltpu.roll(b, step, axis), a),
            jnp.where(keep, b, pltpu.roll(a, back, axis)),
        )

    def first_pass(v, carry):
        for c in range(2):
            x = [state[c, v + quarter * k] for k in range(4)]
            x[0], x[2] = swap(x[0], x[2], high4, high4, 4, 0)
            x[1], x[3] = swap(x[1], x[3], high4, high4, 4, 0)
            for k in (0, 2):
                a, b = swap(x[k], x[k + 1], odd_lane, odd_lane, 1, 1)
                x[k], x[k + 1] = swap(a, b, odd_sub, odd_sub, 1, 0)
            for k in range(4):
                mixed[c, v + quarter * k] = x[k]
        return carry

    lax.fori_loop(0, quarter, first_pass, 0, unroll=32)

    pairs = width // 2
    order = (
        jnp.where(outer, far, beside),
        jnp.where(outer, across, plane),
        jnp.where(outer, beside, far),
        jnp.where(outer, plane, across),
    )

    def target(k):
        at = k // chips
        zone = order[3]
        for i in (2, 1, 0):
            zone = jnp.where(at == i, order[i], zone)
        return zone, jnp.bitwise_xor(chip, chips - 1 - lax.rem(k, chips))

    def pack(k, carry):
        zone, where = target(k)
        owner = zone * chips + where
        for c in range(2):
            for p in range(pairs):
                u = owner * pairs + p
                low = jnp.bitwise_and(u, stride - 1)
                first = 2 * u - low
                a = mixed[c, first]
                b = mixed[c, first + stride]
                a, b = swap(a, b, lane_hit, lane_keep, lane_step, 1)
                a, b = swap(a, b, sub_hit, sub_keep, 2, 0)
                for w, value in enumerate((a, b)):
                    column = (c * width + 2 * p + w) * 128
                    send[owner, :, column : column + 128] = value
        return carry

    together = min(chips, 4)
    lax.fori_loop(0, chips, pack, 0, unroll=together)
    pl.semaphore_wait(barrier, n - 1)

    def send_chunk(k, carry):
        zone, where = target(k)
        owner = zone * chips + where
        device = zone * devs + 2 * where + 1

        @pl.when(device != me)
        def _():
            pltpu.make_async_remote_copy(
                src_ref=send.at[owner], dst_ref=recv.at[me], send_sem=send_sem,
                recv_sem=recv_sem.at[plane], device_id=(device,), device_id_type=MESH,
            ).start()

        @pl.when(device == me)
        def _():
            pltpu.make_async_copy(send.at[owner], recv.at[me], recv_sem.at[plane]).start()

        return carry

    def send_and_pack(i, carry):
        lax.fori_loop(i * chips, (i + 1) * chips, send_chunk, 0)

        def pack_next(k, carry):
            return pack((i + 1) * chips + k, carry)

        lax.fori_loop(0, chips, pack_next, 0, unroll=together)
        return carry

    lax.fori_loop(0, PLANES - 1, send_and_pack, 0)
    lax.fori_loop(owners - chips, owners, send_chunk, 0)

    depth = width * 128
    block = 8 * devs
    wide = max(block, 128)
    ratio = wide // block

    def split(x):
        high = x.astype(jnp.bfloat16)
        return high, (x - high.astype(jnp.float32)).astype(jnp.bfloat16)

    def dot(x, y):
        return lax.dot_general(x, y, (((1,), (1,)), ((), ())), preferred_element_type=jnp.float32)

    def stacked(x):
        return jnp.concatenate(
            [x, jnp.concatenate([x[:, depth:], -x[:, :depth]], axis=1)], axis=0
        )

    def arrival(s):
        second = jnp.where(outer, beside, far)
        third = jnp.where(outer, far, beside)
        return jnp.where(
            s == 0, plane, jnp.where(s == 1, second, jnp.where(s == 2, third, across))
        )

    def gram(s, carry):
        zone = arrival(s)
        mine = pl.ds(zone * devs, devs)
        lines = pl.ds(pl.multiple_of(zone * block, block), block)
        came = recv.at[mine]
        pltpu.make_async_copy(came, came, recv_sem.at[zone]).wait()
        high, low = split(recv[mine].reshape(block, 2 * depth))
        high_ref[lines] = high
        low_ref[lines] = low
        left_h = stacked(high)
        left_l = stacked(low)
        right_h = high_ref[...]
        result = dot(left_h, right_h) + (dot(left_h, low_ref[...]) + dot(left_l, right_h))
        column = pl.ds(pl.multiple_of(zone // ratio * wide, wide), wide)
        for c in range(2):
            value = result[c * block : (c + 1) * block]
            part[mine, :, c * full : (c + 1) * full] = value.reshape(devs, 8, full)
            if c == 1:
                value = -value
            if ratio > 1:
                slot = lax.rem(zone, ratio)
                value = jnp.concatenate(
                    [jnp.where(slot == r, value, 0.0) for r in range(ratio)], axis=0
                )
            turned_ref[c] = value.T.reshape(n, 8, wide)

        def mirror(e, carry):
            there = pl.ds(arrival(e) * devs, devs)
            for c in range(2):
                at = pl.ds(pl.multiple_of(c * full + zone // ratio * wide, wide), wide)
                part[there, :, at] = part[there, :, at] + turned_ref[c, there]
            return carry

        lax.fori_loop(0, s, mirror, 0)
        return carry

    def send_rows(zone, slot, ready):
        def one(k, carry):
            at = jnp.bitwise_xor(lax.rem(me, devs), devs - 1 - k)
            device = zone * devs + at
            ready(device)

            @pl.when(device != me)
            def _():
                pltpu.make_async_remote_copy(
                    src_ref=part.at[device], dst_ref=rows.at[slot, chip], send_sem=row_send,
                    recv_sem=row_recv.at[slot], device_id=(device,), device_id_type=MESH,
                ).start()

            @pl.when(device == me)
            def _():
                pltpu.make_async_copy(
                    part.at[device], rows.at[slot, chip], row_recv.at[slot]
                ).start()

            return carry

        lax.fori_loop(0, devs, one, 0)

    def add_chain(device):
        part[device] = part[device] + chain[device]

    @pl.when(core == 1)
    def _():
        high_ref[...] = jnp.zeros_like(high_ref)
        low_ref[...] = jnp.zeros_like(low_ref)
        lax.fori_loop(0, PLANES, gram, 0)

        @pl.when(outer)
        def _():
            for i, zone in enumerate((far, across, beside)):
                mine = pl.ds(zone * devs, devs)
                pltpu.make_async_remote_copy(
                    src_ref=part.at[mine], dst_ref=chain.at[mine], send_sem=row_send,
                    recv_sem=chain_sem.at[i], device_id=(beside * devs + 2 * chip + 1,),
                    device_id_type=MESH,
                ).start()
            send_rows(plane, 0, lambda device: None)

        @pl.when(inner)
        def _():
            send_rows(beside, 1, lambda device: None)
            for i, (zone, slot) in enumerate(((far, 2), (across, 2), (plane, 0))):
                came = chain.at[pl.ds(zone * devs, devs)]
                pltpu.make_async_copy(came, came, chain_sem.at[i]).wait()
                send_rows(zone, slot, add_chain)

    def gathered(slot):
        pltpu.make_async_copy(rows.at[slot], rows.at[slot], row_recv.at[slot]).wait()
        total = rows[slot, 0]
        for k in range(1, chips):
            total = total + rows[slot, k]
        return total

    out_ref[...] = gathered(0)

    @pl.when(outer)
    def _():
        out_ref[...] = out_ref[...] + gathered(1)

    out_ref[...] = (out_ref[...] + gathered(2)) * scale

    rest = send.at[pl.ds(0, owners - 1)]
    pltpu.make_async_copy(rest, rest, send_sem).wait()

    @pl.when(core == 0)
    def _():
        pltpu.make_async_copy(send.at[0], send.at[0], send_sem).wait()

    @pl.when(core == 1)
    def _():
        sent = part.at[pl.ds(0, n - 1)]
        pltpu.make_async_copy(sent, sent, row_send).wait()


def local(n, state_real, state_imag, subsystem):
    amps = state_real.shape[0]
    vregs = amps // 1024
    owners = n // 2
    width = vregs // owners
    full = 8 * n
    devs = n // PLANES
    wide = max(8 * devs, 128)
    chunk = (8, 2 * width * 128)
    out = pl.pallas_call(
        functools.partial(exchange_kernel, n, 8.0 / amps),
        out_shape=pltpu.VMEM((8, 2 * full), jnp.float32),
        in_specs=[
            pl.BlockSpec(memory_space=pl.ANY),
            pl.BlockSpec(memory_space=pl.ANY),
            pl.BlockSpec(memory_space=pl.ANY),
        ],
        out_specs=pl.BlockSpec(memory_space=pltpu.VMEM),
        scratch_shapes=[
            pltpu.SMEM((3,), jnp.int32),
            pltpu.VMEM((2, vregs, 8, 128), jnp.float32),
            pltpu.VMEM((2, vregs, 8, 128), jnp.float32),
            pltpu.VMEM((owners,) + chunk, jnp.float32),
            pltpu.VMEM((n,) + chunk, jnp.float32),
            pltpu.VMEM((full, chunk[1]), jnp.bfloat16),
            pltpu.VMEM((full, chunk[1]), jnp.bfloat16),
            pltpu.VMEM((n, 8, 2 * full), jnp.float32),
            pltpu.VMEM((2, n, 8, wide), jnp.float32),
            pltpu.VMEM((n, 8, 2 * full), jnp.float32),
            pltpu.VMEM((3, devs // 2, 8, 2 * full), jnp.float32),
            pltpu.SemaphoreType.DMA((3,)),
            pltpu.SemaphoreType.DMA,
            pltpu.SemaphoreType.DMA((PLANES,)),
            pltpu.SemaphoreType.DMA((3,)),
            pltpu.SemaphoreType.DMA,
            pltpu.SemaphoreType.DMA((3,)),
        ],
        compiler_params=pltpu.CompilerParams(
            collective_id=0, has_side_effects=True, vmem_limit_bytes=56 * 2**20
        ),
    )(subsystem, state_real.reshape(vregs, 8, 128), state_imag.reshape(vregs, 8, 128))
    return out[:, :full], out[:, full:]


def solution(mesh):
    return jax.shard_map(
        functools.partial(local, mesh.shape["dev"]),
        mesh=mesh,
        in_specs=(P("dev"), P("dev"), P()),
        out_specs=(P("dev", None), P("dev", None)),
        check_vma=False,
    )
```

```python
import functools

import jax
import jax.numpy as jnp
from jax import lax
from jax.experimental import pallas as pl
from jax.experimental.pallas import tpu as pltpu
from jax.sharding import PartitionSpec as P

MESH = pl.DeviceIdType.MESH
PLANES = 4


def exchange_kernel(n, scale, sub_hbm, re_hbm, im_hbm, out_ref, sub_ref, state, mixed, send, recv,
                    high_ref, low_ref, part, turned_ref, chain, rows, load_sem, send_sem,
                    recv_sem, chain_sem, row_send, row_recv, present):
    me = lax.axis_index("dev")
    loads = [
        pltpu.make_async_copy(sub_hbm, sub_ref, load_sem.at[2]),
        pltpu.make_async_copy(re_hbm, state.at[0], load_sem.at[0]),
        pltpu.make_async_copy(im_hbm, state.at[1], load_sem.at[1]),
    ]
    for load in loads:
        load.start()
    barrier = pltpu.get_barrier_semaphore()

    @pl.when(lax.rem(me, 2) == 1)
    def _():
        def greet(k, carry):
            pl.semaphore_signal(
                barrier, inc=1, device_id=(jnp.bitwise_xor(me, n - k),), device_id_type=MESH
            )
            return carry

        lax.fori_loop(1, n, greet, 0)

    devs = n // PLANES
    chips = devs // 2
    owners = n // 2
    plane = me // devs
    chip = lax.rem(me, devs) // 2
    core = lax.rem(me, 2)
    low_half = plane < 2
    outer = (plane == 0) | (plane == PLANES - 1)
    inner = jnp.logical_not(outer)
    beside = jnp.bitwise_xor(plane, 1)
    far = jnp.where(low_half, 3, 0)
    across = jnp.where(low_half, 2, 1)

    vregs = state.shape[1]
    quarter = vregs // 4
    bits = vregs.bit_length() - 1
    width = vregs // owners
    full = 8 * n

    for load in loads:
        load.wait()

    lane = lax.broadcasted_iota(jnp.int32, (8, 128), 1)
    sub = lax.broadcasted_iota(jnp.int32, (8, 128), 0)

    mid = sub_ref[1]
    lane_step = jnp.int32(1)
    for b in range(1, 7):
        lane_step = jnp.where(mid == b, 2**b, lane_step)
    top = 10 + bits - 1
    in_lane = (mid < 7) | (mid == top - 1)
    stride = jnp.int32(vregs // 8)
    for b in range(10, top - 1):
        stride = jnp.where(mid == b, 2 ** (b - 10), stride)
    stride = jnp.where(mid == 7, vregs // 4, stride)
    stride = jnp.where(mid == 9, vregs // 2, stride)
    fixed = mid == 8
    lane_on = jnp.where(in_lane, lane_step, 0)
    lane_hit = jnp.bitwise_and(lane, lane_on) != 0
    lane_keep = lane_hit | (jnp.where(in_lane, 0, 1) != jnp.bitwise_and(lane, 0))
    sub_on = jnp.where(fixed, 0, 2)
    sub_hit = jnp.bitwise_and(sub, sub_on) != 0
    sub_keep = sub_hit | (jnp.where(fixed, 1, 0) != jnp.bitwise_and(sub, 0))

    high4 = sub >= 4
    odd_sub = jnp.bitwise_and(sub, 1) != 0
    odd_lane = jnp.bitwise_and(lane, 1) != 0

    def swap(a, b, hit, keep, step, axis):
        size = (8, 128)[axis]
        back = size - step
        return (
            jnp.where(hit, pltpu.roll(b, step, axis), a),
            jnp.where(keep, b, pltpu.roll(a, back, axis)),
        )

    def first_pass(v, carry):
        for c in range(2):
            x = [state[c, v + quarter * k] for k in range(4)]
            x[0], x[2] = swap(x[0], x[2], high4, high4, 4, 0)
            x[1], x[3] = swap(x[1], x[3], high4, high4, 4, 0)
            for k in (0, 2):
                a, b = swap(x[k], x[k + 1], odd_lane, odd_lane, 1, 1)
                x[k], x[k + 1] = swap(a, b, odd_sub, odd_sub, 1, 0)
            for k in range(4):
                mixed[c, v + quarter * k] = x[k]
        return carry

    lax.fori_loop(0, quarter, first_pass, 0, unroll=32)

    pairs = width // 2
    order = (
        far,
        jnp.where(outer, across, beside),
        jnp.where(outer, beside, plane),
        jnp.where(outer, plane, across),
    )

    def target(k):
        at = k // chips
        zone = order[3]
        for i in (2, 1, 0):
            zone = jnp.where(at == i, order[i], zone)
        return zone, jnp.bitwise_xor(chip, chips - 1 - lax.rem(k, chips))

    def pack(k, carry):
        zone, where = target(k)
        owner = zone * chips + where
        for c in range(2):
            for p in range(pairs):
                u = owner * pairs + p
                low = jnp.bitwise_and(u, stride - 1)
                first = 2 * u - low
                a = mixed[c, first]
                b = mixed[c, first + stride]
                a, b = swap(a, b, lane_hit, lane_keep, lane_step, 1)
                a, b = swap(a, b, sub_hit, sub_keep, 2, 0)
                for w, value in enumerate((a, b)):
                    column = (c * width + 2 * p + w) * 128
                    send[owner, :, column : column + 128] = value
        return carry

    together = min(chips, 4)
    lax.fori_loop(0, chips, pack, 0, unroll=together)
    pl.semaphore_wait(barrier, owners - core)

    def send_chunk(k, carry):
        zone, where = target(k)
        owner = zone * chips + where
        device = zone * devs + 2 * where + 1

        @pl.when(device != me)
        def _():
            pltpu.make_async_remote_copy(
                src_ref=send.at[owner], dst_ref=recv.at[me], send_sem=send_sem,
                recv_sem=recv_sem.at[plane], device_id=(device,), device_id_type=MESH,
            ).start()

        @pl.when(device == me)
        def _():
            pltpu.make_async_copy(send.at[owner], recv.at[me], recv_sem.at[plane]).start()

        return carry

    def send_and_pack(i, carry):
        lax.fori_loop(i * chips, (i + 1) * chips, send_chunk, 0)

        def pack_next(k, carry):
            return pack((i + 1) * chips + k, carry)

        lax.fori_loop(0, chips, pack_next, 0, unroll=together)
        return carry

    lax.fori_loop(0, PLANES - 1, send_and_pack, 0)
    lax.fori_loop(owners - chips, owners, send_chunk, 0)

    @pl.when(core == 0)
    def _():
        def tell(k, carry):
            pl.semaphore_signal(
                present, inc=1, device_id=(2 * k + 1,), device_id_type=MESH
            )
            return carry

        lax.fori_loop(0, owners, tell, 0)


    depth = width * 128
    block = 8 * devs
    wide = max(block, 128)
    ratio = wide // block

    def split(x):
        high = x.astype(jnp.bfloat16)
        return high, (x - high.astype(jnp.float32)).astype(jnp.bfloat16)

    def dot(x, y):
        return lax.dot_general(x, y, (((1,), (1,)), ((), ())), preferred_element_type=jnp.float32)

    def stacked(x):
        return jnp.concatenate(
            [x, jnp.concatenate([x[:, depth:], -x[:, :depth]], axis=1)], axis=0
        )

    def arrival(s):
        second = jnp.where(outer, beside, far)
        third = jnp.where(outer, far, beside)
        return jnp.where(
            s == 0, plane, jnp.where(s == 1, second, jnp.where(s == 2, third, across))
        )

    def gram(s, carry):
        zone = arrival(s)
        mine = pl.ds(zone * devs, devs)
        lines = pl.ds(pl.multiple_of(zone * block, block), block)
        came = recv.at[mine]
        pltpu.make_async_copy(came, came, recv_sem.at[zone]).wait()
        high, low = split(recv[mine].reshape(block, 2 * depth))
        high_ref[lines] = high
        low_ref[lines] = low
        left_h = stacked(high)
        both = dot(jnp.concatenate([left_h, stacked(low)], axis=0), high_ref[...])
        result = both[: 2 * block] + (both[2 * block :] + dot(left_h, low_ref[...]))
        column = pl.ds(pl.multiple_of(zone // ratio * wide, wide), wide)
        for c in range(2):
            value = result[c * block : (c + 1) * block]
            part[mine, :, c * full : (c + 1) * full] = value.reshape(devs, 8, full)
            if c == 1:
                value = -value
            if ratio > 1:
                slot = lax.rem(zone, ratio)
                value = jnp.concatenate(
                    [jnp.where(slot == r, value, 0.0) for r in range(ratio)], axis=0
                )
            turned_ref[c] = value.T.reshape(n, 8, wide)

        def mirror(e, carry):
            there = pl.ds(arrival(e) * devs, devs)
            for c in range(2):
                at = pl.ds(pl.multiple_of(c * full + zone // ratio * wide, wide), wide)
                part[there, :, at] = part[there, :, at] + turned_ref[c, there]
            return carry

        lax.fori_loop(0, s, mirror, 0)
        return carry

    def send_rows(zone, slot, ready):
        def one(k, carry):
            device = zone * devs + k
            ready(device)

            @pl.when(device != me)
            def _():
                pltpu.make_async_remote_copy(
                    src_ref=part.at[device], dst_ref=rows.at[slot, chip], send_sem=row_send,
                    recv_sem=row_recv.at[slot], device_id=(device,), device_id_type=MESH,
                ).start()

            @pl.when(device == me)
            def _():
                pltpu.make_async_copy(
                    part.at[device], rows.at[slot, chip], row_recv.at[slot]
                ).start()

            return carry

        lax.fori_loop(0, devs, one, 0)

    def add_chain(device):
        part[device] = part[device] + chain[device]

    @pl.when(core == 1)
    def _():
        pl.semaphore_wait(present, owners)
        high_ref[...] = jnp.zeros_like(high_ref)
        low_ref[...] = jnp.zeros_like(low_ref)
        lax.fori_loop(0, PLANES, gram, 0)

        @pl.when(outer)
        def _():
            for i, zone in enumerate((far, across, beside)):
                mine = pl.ds(zone * devs, devs)
                pltpu.make_async_remote_copy(
                    src_ref=part.at[mine], dst_ref=chain.at[mine], send_sem=row_send,
                    recv_sem=chain_sem.at[i], device_id=(beside * devs + 2 * chip + 1,),
                    device_id_type=MESH,
                ).start()
            send_rows(plane, 0, lambda device: None)

        @pl.when(inner)
        def _():
            for i, (zone, slot) in enumerate(((far, 2), (across, 2), (plane, 0))):
                came = chain.at[pl.ds(zone * devs, devs)]
                pltpu.make_async_copy(came, came, chain_sem.at[i]).wait()
                send_rows(zone, slot, add_chain)
                if i == 0:
                    send_rows(beside, 1, lambda device: None)

    def gathered(slot):
        pltpu.make_async_copy(rows.at[slot], rows.at[slot], row_recv.at[slot]).wait()
        total = rows[slot, 0]
        for k in range(1, chips):
            total = total + rows[slot, k]
        return total

    out_ref[...] = gathered(0)

    @pl.when(outer)
    def _():
        out_ref[...] = out_ref[...] + gathered(1)

    out_ref[...] = (out_ref[...] + gathered(2)) * scale

    rest = send.at[pl.ds(0, owners - 1)]
    pltpu.make_async_copy(rest, rest, send_sem).wait()

    @pl.when(core == 0)
    def _():
        pltpu.make_async_copy(send.at[0], send.at[0], send_sem).wait()

    @pl.when(core == 1)
    def _():
        sent = part.at[pl.ds(0, n - 1)]
        pltpu.make_async_copy(sent, sent, row_send).wait()


def local(n, state_real, state_imag, subsystem):
    amps = state_real.shape[0]
    vregs = amps // 1024
    owners = n // 2
    width = vregs // owners
    full = 8 * n
    devs = n // PLANES
    wide = max(8 * devs, 128)
    chunk = (8, 2 * width * 128)
    out = pl.pallas_call(
        functools.partial(exchange_kernel, n, 8.0 / amps),
        out_shape=pltpu.VMEM((8, 2 * full), jnp.float32),
        in_specs=[
            pl.BlockSpec(memory_space=pl.ANY),
            pl.BlockSpec(memory_space=pl.ANY),
            pl.BlockSpec(memory_space=pl.ANY),
        ],
        out_specs=pl.BlockSpec(memory_space=pltpu.VMEM),
        scratch_shapes=[
            pltpu.SMEM((3,), jnp.int32),
            pltpu.VMEM((2, vregs, 8, 128), jnp.float32),
            pltpu.VMEM((2, vregs, 8, 128), jnp.float32),
            pltpu.VMEM((owners,) + chunk, jnp.float32),
            pltpu.VMEM((n,) + chunk, jnp.float32),
            pltpu.VMEM((full, chunk[1]), jnp.bfloat16),
            pltpu.VMEM((full, chunk[1]), jnp.bfloat16),
            pltpu.VMEM((n, 8, 2 * full), jnp.float32),
            pltpu.VMEM((2, n, 8, wide), jnp.float32),
            pltpu.VMEM((n, 8, 2 * full), jnp.float32),
            pltpu.VMEM((3, devs // 2, 8, 2 * full), jnp.float32),
            pltpu.SemaphoreType.DMA((3,)),
            pltpu.SemaphoreType.DMA,
            pltpu.SemaphoreType.DMA((PLANES,)),
            pltpu.SemaphoreType.DMA((3,)),
            pltpu.SemaphoreType.DMA,
            pltpu.SemaphoreType.DMA((3,)),
            pltpu.SemaphoreType.REGULAR,
        ],
        compiler_params=pltpu.CompilerParams(
            collective_id=0, has_side_effects=True, vmem_limit_bytes=56 * 2**20
        ),
    )(subsystem, state_real.reshape(vregs, 8, 128), state_imag.reshape(vregs, 8, 128))
    return out[:, :full], out[:, full:]


def solution(mesh):
    return jax.shard_map(
        functools.partial(local, mesh.shape["dev"]),
        mesh=mesh,
        in_specs=(P("dev"), P("dev"), P()),
        out_specs=(P("dev", None), P("dev", None)),
        check_vma=False,
    )
```

```python
import functools

import jax
import jax.numpy as jnp
from jax import lax
from jax.experimental import pallas as pl
from jax.experimental.pallas import tpu as pltpu
from jax.sharding import PartitionSpec as P

MESH = pl.DeviceIdType.MESH
PLANES = 4


def exchange_kernel(n, scale, sub_hbm, re_hbm, im_hbm, out_ref, sub_ref, state, mixed, send, recv,
                    high_ref, low_ref, part, turned_ref, chain, rows, load_sem, send_sem,
                    recv_sem, chain_sem, row_send, row_recv, present):
    me = lax.axis_index("dev")
    loads = [
        pltpu.make_async_copy(sub_hbm, sub_ref, load_sem.at[2]),
        pltpu.make_async_copy(re_hbm, state.at[0], load_sem.at[0]),
        pltpu.make_async_copy(im_hbm, state.at[1], load_sem.at[1]),
    ]
    for load in loads:
        load.start()
    barrier = pltpu.get_barrier_semaphore()

    @pl.when(lax.rem(me, 2) == 1)
    def _():
        def greet(k, carry):
            pl.semaphore_signal(
                barrier, inc=1, device_id=(jnp.bitwise_xor(me, n - k),), device_id_type=MESH
            )
            return carry

        lax.fori_loop(1, n, greet, 0)

    devs = n // PLANES
    chips = devs // 2
    owners = n // 2
    plane = me // devs
    chip = lax.rem(me, devs) // 2
    core = lax.rem(me, 2)
    low_half = plane < 2
    outer = (plane == 0) | (plane == PLANES - 1)
    inner = jnp.logical_not(outer)
    beside = jnp.bitwise_xor(plane, 1)
    far = jnp.where(low_half, 3, 0)
    across = jnp.where(low_half, 2, 1)

    vregs = state.shape[1]
    quarter = vregs // 4
    bits = vregs.bit_length() - 1
    width = vregs // owners
    full = 8 * n

    loads[0].wait()

    lane = lax.broadcasted_iota(jnp.int32, (8, 128), 1)
    sub = lax.broadcasted_iota(jnp.int32, (8, 128), 0)

    mid = sub_ref[1]
    lane_step = jnp.int32(1)
    for b in range(1, 7):
        lane_step = jnp.where(mid == b, 2**b, lane_step)
    top = 10 + bits - 1
    in_lane = (mid < 7) | (mid == top - 1)
    stride = jnp.int32(vregs // 8)
    for b in range(10, top - 1):
        stride = jnp.where(mid == b, 2 ** (b - 10), stride)
    stride = jnp.where(mid == 7, vregs // 4, stride)
    stride = jnp.where(mid == 9, vregs // 2, stride)
    fixed = mid == 8
    lane_on = jnp.where(in_lane, lane_step, 0)
    lane_hit = jnp.bitwise_and(lane, lane_on) != 0
    lane_keep = lane_hit | (jnp.where(in_lane, 0, 1) != jnp.bitwise_and(lane, 0))
    sub_on = jnp.where(fixed, 0, 2)
    sub_hit = jnp.bitwise_and(sub, sub_on) != 0
    sub_keep = sub_hit | (jnp.where(fixed, 1, 0) != jnp.bitwise_and(sub, 0))

    high4 = sub >= 4
    odd_sub = jnp.bitwise_and(sub, 1) != 0
    odd_lane = jnp.bitwise_and(lane, 1) != 0

    def swap(a, b, hit, keep, step, axis):
        size = (8, 128)[axis]
        back = size - step
        return (
            jnp.where(hit, pltpu.roll(b, step, axis), a),
            jnp.where(keep, b, pltpu.roll(a, back, axis)),
        )

    for c in range(2):
        loads[1 + c].wait()

        def first_pass(v, carry):
            x = [state[c, v + quarter * k] for k in range(4)]
            x[0], x[2] = swap(x[0], x[2], high4, high4, 4, 0)
            x[1], x[3] = swap(x[1], x[3], high4, high4, 4, 0)
            for k in (0, 2):
                a, b = swap(x[k], x[k + 1], odd_lane, odd_lane, 1, 1)
                x[k], x[k + 1] = swap(a, b, odd_sub, odd_sub, 1, 0)
            for k in range(4):
                mixed[c, v + quarter * k] = x[k]
            return carry

        lax.fori_loop(0, quarter, first_pass, 0, unroll=32)

    pairs = width // 2
    tiles = width // 2
    depth = tiles * 128
    order = (
        far,
        jnp.where(outer, across, beside),
        jnp.where(outer, beside, plane),
        jnp.where(outer, plane, across),
    )

    def target(k):
        at = k // chips
        zone = order[3]
        for i in (2, 1, 0):
            zone = jnp.where(at == i, order[i], zone)
        return zone, jnp.bitwise_xor(chip, chips - 1 - lax.rem(k, chips))

    def pack(k, carry):
        zone, where = target(k)
        owner = zone * chips + where
        for c in range(2):
            for p in range(pairs):
                u = owner * pairs + p
                low = jnp.bitwise_and(u, stride - 1)
                first = 2 * u - low
                a = mixed[c, first]
                b = mixed[c, first + stride]
                a, b = swap(a, b, lane_hit, lane_keep, lane_step, 1)
                a, b = swap(a, b, sub_hit, sub_keep, 2, 0)
                for w, value in enumerate((a, b)):
                    half, tile = divmod(2 * p + w, tiles)
                    column = (c * tiles + tile) * 128
                    send[owner, half, :, column : column + 128] = value
        return carry

    together = min(chips, 4)
    lax.fori_loop(0, chips, pack, 0, unroll=together)
    pl.semaphore_wait(barrier, owners - core)

    def send_group(i):
        def send_chunk(k, carry):
            zone, where = target(i * chips + lax.rem(k, chips))
            half = k // chips
            owner = zone * chips + where
            device = zone * devs + 2 * where + 1

            @pl.when(device != me)
            def _():
                pltpu.make_async_remote_copy(
                    src_ref=send.at[owner, half], dst_ref=recv.at[half, me], send_sem=send_sem,
                    recv_sem=recv_sem.at[plane, half], device_id=(device,), device_id_type=MESH,
                ).start()

            @pl.when(device == me)
            def _():
                pltpu.make_async_copy(
                    send.at[owner, half], recv.at[half, me], recv_sem.at[plane, half]
                ).start()

            return carry

        lax.fori_loop(0, 2 * chips, send_chunk, 0)

    def send_and_pack(i, carry):
        send_group(i)

        def pack_next(k, carry):
            return pack((i + 1) * chips + k, carry)

        lax.fori_loop(0, chips, pack_next, 0, unroll=together)
        return carry

    lax.fori_loop(0, PLANES - 1, send_and_pack, 0)
    send_group(PLANES - 1)

    @pl.when(core == 0)
    def _():
        def tell(k, carry):
            pl.semaphore_signal(
                present, inc=1, device_id=(2 * k + 1,), device_id_type=MESH
            )
            return carry

        lax.fori_loop(0, owners, tell, 0)


    block = 8 * devs
    wide = max(block, 128)
    ratio = wide // block
    columns = full // 2

    def split(x):
        high = x.astype(jnp.bfloat16)
        return high, (x - high.astype(jnp.float32)).astype(jnp.bfloat16)

    def dot(x, y):
        return lax.dot_general(x, y, (((1,), (1,)), ((), ())), preferred_element_type=jnp.float32)

    def stacked(x):
        return jnp.concatenate(
            [x, jnp.concatenate([x[:, depth:], -x[:, :depth]], axis=1)], axis=0
        )

    def arrival(s):
        second = jnp.where(outer, far, beside)
        third = jnp.where(outer, across, far)
        last = jnp.where(outer, beside, across)
        return jnp.where(
            s == 0, plane, jnp.where(s == 1, second, jnp.where(s == 2, third, last))
        )

    def gram(step, carry):
        zone = arrival(step // 2)
        half = lax.rem(step, 2)
        mine = pl.ds(zone * devs, devs)
        lines = pl.ds(pl.multiple_of(zone * block, block), block)
        came = recv.at[half, mine]
        pltpu.make_async_copy(came, came, recv_sem.at[zone, half]).wait()
        high, low = split(recv[half, mine].reshape(block, 2 * depth))
        high_ref[half, lines] = high
        low_ref[half, lines] = low
        left_h = stacked(high)
        both = dot(jnp.concatenate([left_h, stacked(low)], axis=0), high_ref[half])
        result = both[: 2 * block] + (both[2 * block :] + dot(left_h, low_ref[half]))
        start = lax.rem(zone * block, columns) // wide * wide
        for c in range(2):
            value = result[c * block : (c + 1) * block]
            here = slice(c * columns, (c + 1) * columns)
            for side in range(2):
                piece = value[:, side * columns : (side + 1) * columns]
                part[mine, side, :, here] = part[mine, side, :, here] + piece.reshape(
                    devs, 8, columns
                )
            if c == 1:
                value = -value
            if ratio > 1:
                slot = lax.rem(zone, ratio)
                value = jnp.concatenate(
                    [jnp.where(slot == r, value, 0.0) for r in range(ratio)], axis=0
                )
            turned_ref[c] = value.T.reshape(n, 8, wide)

        def mirror(e, carry):
            there = pl.ds(arrival(e) * devs, devs)
            for c in range(2):
                at = pl.ds(pl.multiple_of(c * columns + start, 128), wide)
                part[there, zone // 2, :, at] = (
                    part[there, zone // 2, :, at] + turned_ref[c, there]
                )
            return carry

        lax.fori_loop(0, step // 2, mirror, 0)
        return carry

    def send_rows(zone, slot, half=None, ready=None):
        def one(k, carry):
            device = zone * devs + k
            if ready is not None:
                ready(device)
            if half is None:
                source, target_rows = part.at[device], rows.at[slot, chip]
            else:
                source, target_rows = part.at[device, half], rows.at[slot, chip, half]

            @pl.when(device != me)
            def _():
                pltpu.make_async_remote_copy(
                    src_ref=source, dst_ref=target_rows, send_sem=row_send,
                    recv_sem=row_recv.at[slot], device_id=(device,), device_id_type=MESH,
                ).start()

            @pl.when(device == me)
            def _():
                pltpu.make_async_copy(source, target_rows, row_recv.at[slot]).start()

            return carry

        lax.fori_loop(0, devs, one, 0)

    def add_chain(device):
        part[device] = part[device] + chain[device]

    @pl.when(core == 1)
    def _():
        pl.semaphore_wait(present, owners)
        high_ref[...] = jnp.zeros_like(high_ref)
        low_ref[...] = jnp.zeros_like(low_ref)
        part[...] = jnp.zeros_like(part)
        lax.fori_loop(0, 2 * PLANES - 2, gram, 0)
        near = plane // 2

        @pl.when(inner)
        def _():
            send_rows(beside, 1, near)
            send_rows(plane, 0, near)

        lax.fori_loop(2 * PLANES - 2, 2 * PLANES, gram, 0)

        @pl.when(outer)
        def _():
            for i, zone in enumerate((far, across)):
                mine = pl.ds(zone * devs, devs)
                pltpu.make_async_remote_copy(
                    src_ref=part.at[mine], dst_ref=chain.at[mine], send_sem=row_send,
                    recv_sem=chain_sem.at[i], device_id=(beside * devs + 2 * chip + 1,),
                    device_id_type=MESH,
                ).start()
            send_rows(beside, 1)
            send_rows(plane, 0)

        @pl.when(inner)
        def _():
            for i, zone in enumerate((far, across)):
                came = chain.at[pl.ds(zone * devs, devs)]
                pltpu.make_async_copy(came, came, chain_sem.at[i]).wait()
                send_rows(zone, 2, ready=add_chain)
                if i == 0:
                    send_rows(beside, 1, 1 - near)
            send_rows(plane, 0, 1 - near)

    def gathered(slot):
        pltpu.make_async_copy(rows.at[slot], rows.at[slot], row_recv.at[slot]).wait()
        total = rows[slot, 0]
        for k in range(1, chips):
            total = total + rows[slot, k]
        return total

    total = (gathered(0) + gathered(1) + gathered(2)) * scale
    for side in range(2):
        for c in range(2):
            at = c * full + side * columns
            out_ref[:, at : at + columns] = total[side, :, c * columns : (c + 1) * columns]

    rest = send.at[pl.ds(0, owners - 1)]
    pltpu.make_async_copy(rest, rest, send_sem).wait()

    @pl.when(core == 0)
    def _():
        pltpu.make_async_copy(send.at[0], send.at[0], send_sem).wait()

    @pl.when(core == 1)
    def _():
        sent = part.at[pl.ds(0, n - 1)]
        pltpu.make_async_copy(sent, sent, row_send).wait()


def local(n, state_real, state_imag, subsystem):
    amps = state_real.shape[0]
    vregs = amps // 1024
    owners = n // 2
    width = vregs // owners
    full = 8 * n
    devs = n // PLANES
    wide = max(8 * devs, 128)
    chunk = (8, width * 128)
    out = pl.pallas_call(
        functools.partial(exchange_kernel, n, 8.0 / amps),
        out_shape=pltpu.VMEM((8, 2 * full), jnp.float32),
        in_specs=[
            pl.BlockSpec(memory_space=pl.ANY),
            pl.BlockSpec(memory_space=pl.ANY),
            pl.BlockSpec(memory_space=pl.ANY),
        ],
        out_specs=pl.BlockSpec(memory_space=pltpu.VMEM),
        scratch_shapes=[
            pltpu.SMEM((3,), jnp.int32),
            pltpu.VMEM((2, vregs, 8, 128), jnp.float32),
            pltpu.VMEM((2, vregs, 8, 128), jnp.float32),
            pltpu.VMEM((owners, 2) + chunk, jnp.float32),
            pltpu.VMEM((2, n) + chunk, jnp.float32),
            pltpu.VMEM((2, full, chunk[1]), jnp.bfloat16),
            pltpu.VMEM((2, full, chunk[1]), jnp.bfloat16),
            pltpu.VMEM((n, 2, 8, full), jnp.float32),
            pltpu.VMEM((2, n, 8, wide), jnp.float32),
            pltpu.VMEM((n, 2, 8, full), jnp.float32),
            pltpu.VMEM((3, devs // 2, 2, 8, full), jnp.float32),
            pltpu.SemaphoreType.DMA((3,)),
            pltpu.SemaphoreType.DMA,
            pltpu.SemaphoreType.DMA((PLANES, 2)),
            pltpu.SemaphoreType.DMA((2,)),
            pltpu.SemaphoreType.DMA,
            pltpu.SemaphoreType.DMA((3,)),
            pltpu.SemaphoreType.REGULAR,
        ],
        compiler_params=pltpu.CompilerParams(
            collective_id=0, has_side_effects=True, vmem_limit_bytes=56 * 2**20
        ),
    )(subsystem, state_real.reshape(vregs, 8, 128), state_imag.reshape(vregs, 8, 128))
    return out[:, :full], out[:, full:]


def solution(mesh):
    return jax.shard_map(
        functools.partial(local, mesh.shape["dev"]),
        mesh=mesh,
        in_specs=(P("dev"), P("dev"), P()),
        out_specs=(P("dev", None), P("dev", None)),
        check_vma=False,
    )
```

```python
import functools

import jax
import jax.numpy as jnp
from jax import lax
from jax.experimental import pallas as pl
from jax.experimental.pallas import tpu as pltpu
from jax.sharding import PartitionSpec as P

MESH = pl.DeviceIdType.MESH
PLANES = 4


def exchange_kernel(n, scale, sub_hbm, re_hbm, im_hbm, out_ref, sub_ref, state, mixed, send, recv,
                    high_ref, low_ref, part, turned_ref, chain, rows, load_sem, send_sem,
                    recv_sem, chain_sem, row_send, row_recv, present, outer_in, go):
    me = lax.axis_index("dev")
    loads = [
        pltpu.make_async_copy(sub_hbm, sub_ref, load_sem.at[2]),
        pltpu.make_async_copy(re_hbm, state.at[0], load_sem.at[0]),
        pltpu.make_async_copy(im_hbm, state.at[1], load_sem.at[1]),
    ]
    for load in loads:
        load.start()
    barrier = pltpu.get_barrier_semaphore()

    devs = n // PLANES
    chips = devs // 2
    owners = n // 2
    plane = me // devs
    chip = lax.rem(me, devs) // 2
    core = lax.rem(me, 2)
    low_half = plane < 2
    outer = (plane == 0) | (plane == PLANES - 1)
    inner = jnp.logical_not(outer)
    beside = jnp.bitwise_xor(plane, 1)
    far = jnp.where(low_half, 3, 0)
    across = jnp.where(low_half, 2, 1)

    mate = jnp.bitwise_xor(me, 1)

    def signal(sem, device):
        pl.semaphore_signal(sem, inc=1, device_id=(device,), device_id_type=MESH)

    @pl.when(inner & (core == 1))
    def _():
        def greet(k, carry):
            signal(barrier, jnp.bitwise_xor(me, n - k))
            return carry

        lax.fori_loop(1, n, greet, 0)

    @pl.when(outer | (core == 0))
    def _():
        signal(barrier, mate)

    vregs = state.shape[1]
    quarter = vregs // 4
    bits = vregs.bit_length() - 1
    width = vregs // owners
    full = 8 * n

    loads[0].wait()

    lane = lax.broadcasted_iota(jnp.int32, (8, 128), 1)
    sub = lax.broadcasted_iota(jnp.int32, (8, 128), 0)

    mid = sub_ref[1]
    lane_step = jnp.int32(1)
    for b in range(1, 7):
        lane_step = jnp.where(mid == b, 2**b, lane_step)
    top = 10 + bits - 1
    in_lane = (mid < 7) | (mid == top - 1)
    stride = jnp.int32(vregs // 8)
    for b in range(10, top - 1):
        stride = jnp.where(mid == b, 2 ** (b - 10), stride)
    stride = jnp.where(mid == 7, vregs // 4, stride)
    stride = jnp.where(mid == 9, vregs // 2, stride)
    fixed = mid == 8
    lane_on = jnp.where(in_lane, lane_step, 0)
    lane_hit = jnp.bitwise_and(lane, lane_on) != 0
    lane_keep = lane_hit | (jnp.where(in_lane, 0, 1) != jnp.bitwise_and(lane, 0))
    sub_on = jnp.where(fixed, 0, 2)
    sub_hit = jnp.bitwise_and(sub, sub_on) != 0
    sub_keep = sub_hit | (jnp.where(fixed, 1, 0) != jnp.bitwise_and(sub, 0))

    high4 = sub >= 4
    odd_sub = jnp.bitwise_and(sub, 1) != 0
    odd_lane = jnp.bitwise_and(lane, 1) != 0

    def swap(a, b, hit, keep, step, axis):
        size = (8, 128)[axis]
        back = size - step
        return (
            jnp.where(hit, pltpu.roll(b, step, axis), a),
            jnp.where(keep, b, pltpu.roll(a, back, axis)),
        )

    for c in range(2):
        loads[1 + c].wait()

        def first_pass(v, carry):
            x = [state[c, v + quarter * k] for k in range(4)]
            x[0], x[2] = swap(x[0], x[2], high4, high4, 4, 0)
            x[1], x[3] = swap(x[1], x[3], high4, high4, 4, 0)
            for k in (0, 2):
                a, b = swap(x[k], x[k + 1], odd_lane, odd_lane, 1, 1)
                x[k], x[k + 1] = swap(a, b, odd_sub, odd_sub, 1, 0)
            for k in range(4):
                mixed[c, v + quarter * k] = x[k]
            return carry

        lax.fori_loop(0, quarter, first_pass, 0, unroll=32)

    pairs = width // 2
    tiles = width // 2
    depth = tiles * 128
    def target(zone, k):
        return zone * chips + jnp.bitwise_xor(chip, chips - 1 - k)

    def pack(owner):
        for c in range(2):
            for p in range(pairs):
                u = owner * pairs + p
                low = jnp.bitwise_and(u, stride - 1)
                first = 2 * u - low
                a = mixed[c, first]
                b = mixed[c, first + stride]
                a, b = swap(a, b, lane_hit, lane_keep, lane_step, 1)
                a, b = swap(a, b, sub_hit, sub_keep, 2, 0)
                for w, value in enumerate((a, b)):
                    half, tile = divmod(2 * p + w, tiles)
                    column = (c * tiles + tile) * 128
                    send[owner, half, :, column : column + 128] = value

    def pack_group(zone, start):
        def one(k, carry):
            pack(target(zone, k))
            return carry

        lax.fori_loop(start, chips, one, 0, unroll=4 - start if chips >= 4 else 1)

    def send_group(zone, start, stop):
        count = stop - start

        def one(k, carry):
            owner = target(zone, start + lax.rem(k, count))
            half = k // count
            device = 2 * owner + 1

            @pl.when(device != me)
            def _():
                pltpu.make_async_remote_copy(
                    src_ref=send.at[owner, half], dst_ref=recv.at[half, me], send_sem=send_sem,
                    recv_sem=recv_sem.at[plane, half], device_id=(device,), device_id_type=MESH,
                ).start()

            @pl.when(device == me)
            def _():
                pltpu.make_async_copy(
                    send.at[owner, half], recv.at[half, me], recv_sem.at[plane, half]
                ).start()

            return carry

        lax.fori_loop(0, 2 * count, one, 0)

    pack(target(across, 0))
    pl.semaphore_wait(barrier, owners // 2 + jnp.where(outer, 1, 0))

    @pl.when(outer & (core == 1))
    def _():
        def tell(k, carry):
            signal(outer_in, devs + 2 * k + 1)
            return carry

        lax.fori_loop(0, owners // 2, tell, 0)

    send_group(across, 0, 1)
    pack_group(far, 0)

    @pl.when(inner & (core == 1))
    def _():
        pl.semaphore_wait(outer_in, owners // 2)
        signal(go, mate)
        signal(go, beside * devs + 2 * chip + 1)

    @pl.when(outer | (core == 0))
    def _():
        pl.semaphore_wait(go, 1)

    @pl.when(outer & (core == 1))
    def _():
        signal(go, mate)

    send_group(far, 0, chips)
    pack_group(beside, 0)
    send_group(beside, 0, chips)
    pack_group(across, 1)
    send_group(across, 1, chips)
    pack_group(plane, 0)
    send_group(plane, 0, chips)

    @pl.when(core == 0)
    def _():
        def tell(k, carry):
            signal(present, 2 * k + 1)
            return carry

        lax.fori_loop(0, owners, tell, 0)


    block = 8 * devs
    wide = max(block, 128)
    ratio = wide // block
    columns = full // 2

    def split(x):
        high = x.astype(jnp.bfloat16)
        return high, (x - high.astype(jnp.float32)).astype(jnp.bfloat16)

    def dot(x, y):
        return lax.dot_general(x, y, (((1,), (1,)), ((), ())), preferred_element_type=jnp.float32)

    def stacked(x):
        return jnp.concatenate(
            [x, jnp.concatenate([x[:, depth:], -x[:, :depth]], axis=1)], axis=0
        )

    def arrival(s):
        second = jnp.where(outer, far, beside)
        third = jnp.where(outer, across, far)
        last = jnp.where(outer, beside, across)
        return jnp.where(
            s == 0, plane, jnp.where(s == 1, second, jnp.where(s == 2, third, last))
        )

    def gram(step, carry):
        crossed = outer & (step >= 4)
        at = jnp.where(crossed, 2 + lax.rem(step, 2), step // 2)
        half = jnp.where(crossed, step // 2 - 2, lax.rem(step, 2))
        zone = arrival(at)
        mine = pl.ds(zone * devs, devs)
        lines = pl.ds(pl.multiple_of(zone * block, block), block)
        came = recv.at[half, mine]
        pltpu.make_async_copy(came, came, recv_sem.at[zone, half]).wait()
        high, low = split(recv[half, mine].reshape(block, 2 * depth))
        high_ref[half, lines] = high
        low_ref[half, lines] = low
        left_h = stacked(high)
        both = dot(jnp.concatenate([left_h, stacked(low)], axis=0), high_ref[half])
        result = both[: 2 * block] + (both[2 * block :] + dot(left_h, low_ref[half]))
        start = lax.rem(zone * block, columns) // wide * wide
        for c in range(2):
            value = result[c * block : (c + 1) * block]
            here = slice(c * columns, (c + 1) * columns)
            for side in range(2):
                piece = value[:, side * columns : (side + 1) * columns]
                part[mine, side, :, here] = part[mine, side, :, here] + piece.reshape(
                    devs, 8, columns
                )
            if c == 1:
                value = -value
            if ratio > 1:
                slot = lax.rem(zone, ratio)
                value = jnp.concatenate(
                    [jnp.where(slot == r, value, 0.0) for r in range(ratio)], axis=0
                )
            turned_ref[c] = value.T.reshape(n, 8, wide)

        def mirror(e, carry):
            there = pl.ds(arrival(e) * devs, devs)
            for c in range(2):
                span = pl.ds(pl.multiple_of(c * columns + start, 128), wide)
                part[there, zone // 2, :, span] = (
                    part[there, zone // 2, :, span] + turned_ref[c, there]
                )
            return carry

        lax.fori_loop(0, at, mirror, 0)
        return carry

    def send_rows(zone, slot, half=None, ready=None, first=0, last=devs):
        def one(k, carry):
            device = zone * devs + k
            if ready is not None:
                ready(device)
            if half is None:
                source, target_rows = part.at[device], rows.at[slot, chip]
            else:
                source, target_rows = part.at[device, half], rows.at[slot, chip, half]

            @pl.when(device != me)
            def _():
                pltpu.make_async_remote_copy(
                    src_ref=source, dst_ref=target_rows, send_sem=row_send,
                    recv_sem=row_recv.at[slot], device_id=(device,), device_id_type=MESH,
                ).start()

            @pl.when(device == me)
            def _():
                pltpu.make_async_copy(source, target_rows, row_recv.at[slot]).start()

            return carry

        lax.fori_loop(first, last, one, 0)

    def add_chain(device):
        part[device] = part[device] + chain[device]

    @pl.when(core == 1)
    def _():
        pl.semaphore_wait(present, owners)
        high_ref[...] = jnp.zeros_like(high_ref)
        low_ref[...] = jnp.zeros_like(low_ref)
        part[...] = jnp.zeros_like(part)
        lax.fori_loop(0, 2 * PLANES - 2, gram, 0)
        near = plane // 2

        @pl.when(inner)
        def _():
            send_rows(beside, 1, near)
            send_rows(plane, 0, near)

        lax.fori_loop(2 * PLANES - 2, 2 * PLANES, gram, 0)

        @pl.when(outer)
        def _():
            for i in range(4):
                mine = pl.ds((far, across)[i // 2] * devs + i % 2 * chips, chips)
                pltpu.make_async_remote_copy(
                    src_ref=part.at[mine], dst_ref=chain.at[mine], send_sem=row_send,
                    recv_sem=chain_sem.at[i], device_id=(beside * devs + 2 * chip + 1,),
                    device_id_type=MESH,
                ).start()
            send_rows(beside, 1)
            send_rows(plane, 0)

        @pl.when(inner)
        def _():
            send_rows(beside, 1, 1 - near)
            for i in range(4):
                zone, first = (far, across)[i // 2], i % 2 * chips
                came = chain.at[pl.ds(zone * devs + first, chips)]
                pltpu.make_async_copy(came, came, chain_sem.at[i]).wait()
                send_rows(zone, 2, ready=add_chain, first=first, last=first + chips)
            send_rows(plane, 0, 1 - near)

    def gathered(slot):
        pltpu.make_async_copy(rows.at[slot], rows.at[slot], row_recv.at[slot]).wait()
        total = rows[slot, 0]
        for k in range(1, chips):
            total = total + rows[slot, k]
        return total

    total = (gathered(0) + gathered(1) + gathered(2)) * scale
    for side in range(2):
        for c in range(2):
            at = c * full + side * columns
            out_ref[:, at : at + columns] = total[side, :, c * columns : (c + 1) * columns]

    rest = send.at[pl.ds(0, owners - 1)]
    pltpu.make_async_copy(rest, rest, send_sem).wait()

    @pl.when(core == 0)
    def _():
        pltpu.make_async_copy(send.at[0], send.at[0], send_sem).wait()

    @pl.when(core == 1)
    def _():
        sent = part.at[pl.ds(0, n - 1)]
        pltpu.make_async_copy(sent, sent, row_send).wait()


def local(n, state_real, state_imag, subsystem):
    amps = state_real.shape[0]
    vregs = amps // 1024
    owners = n // 2
    width = vregs // owners
    full = 8 * n
    devs = n // PLANES
    wide = max(8 * devs, 128)
    chunk = (8, width * 128)
    out = pl.pallas_call(
        functools.partial(exchange_kernel, n, 8.0 / amps),
        out_shape=pltpu.VMEM((8, 2 * full), jnp.float32),
        in_specs=[
            pl.BlockSpec(memory_space=pl.ANY),
            pl.BlockSpec(memory_space=pl.ANY),
            pl.BlockSpec(memory_space=pl.ANY),
        ],
        out_specs=pl.BlockSpec(memory_space=pltpu.VMEM),
        scratch_shapes=[
            pltpu.SMEM((3,), jnp.int32),
            pltpu.VMEM((2, vregs, 8, 128), jnp.float32),
            pltpu.VMEM((2, vregs, 8, 128), jnp.float32),
            pltpu.VMEM((owners, 2) + chunk, jnp.float32),
            pltpu.VMEM((2, n) + chunk, jnp.float32),
            pltpu.VMEM((2, full, chunk[1]), jnp.bfloat16),
            pltpu.VMEM((2, full, chunk[1]), jnp.bfloat16),
            pltpu.VMEM((n, 2, 8, full), jnp.float32),
            pltpu.VMEM((2, n, 8, wide), jnp.float32),
            pltpu.VMEM((n, 2, 8, full), jnp.float32),
            pltpu.VMEM((3, devs // 2, 2, 8, full), jnp.float32),
            pltpu.SemaphoreType.DMA((3,)),
            pltpu.SemaphoreType.DMA,
            pltpu.SemaphoreType.DMA((PLANES, 2)),
            pltpu.SemaphoreType.DMA((4,)),
            pltpu.SemaphoreType.DMA,
            pltpu.SemaphoreType.DMA((3,)),
            pltpu.SemaphoreType.REGULAR,
            pltpu.SemaphoreType.REGULAR,
            pltpu.SemaphoreType.REGULAR,
        ],
        compiler_params=pltpu.CompilerParams(
            collective_id=0, has_side_effects=True, vmem_limit_bytes=56 * 2**20
        ),
    )(subsystem, state_real.reshape(vregs, 8, 128), state_imag.reshape(vregs, 8, 128))
    return out[:, :full], out[:, full:]


def solution(mesh):
    return jax.shard_map(
        functools.partial(local, mesh.shape["dev"]),
        mesh=mesh,
        in_specs=(P("dev"), P("dev"), P()),
        out_specs=(P("dev", None), P("dev", None)),
        check_vma=False,
    )
```

```python
import functools

import jax
import jax.numpy as jnp
from jax import lax
from jax.experimental import pallas as pl
from jax.experimental.pallas import tpu as pltpu
from jax.sharding import PartitionSpec as P

MESH = pl.DeviceIdType.MESH
PLANES = 4


def exchange_kernel(n, scale, sub_hbm, re_hbm, im_hbm, out_ref, sub_ref, state, mixed, send, recv,
                    high_ref, low_ref, part, turned_ref, chain, rows, load_sem, send_sem,
                    recv_sem, chain_sem, row_send, row_recv, present, outer_in, column_in, go):
    me = lax.axis_index("dev")
    loads = [
        pltpu.make_async_copy(sub_hbm, sub_ref, load_sem.at[2]),
        pltpu.make_async_copy(re_hbm, state.at[0], load_sem.at[0]),
        pltpu.make_async_copy(im_hbm, state.at[1], load_sem.at[1]),
    ]
    for load in loads:
        load.start()
    barrier = pltpu.get_barrier_semaphore()

    devs = n // PLANES
    chips = devs // 2
    owners = n // 2
    plane = me // devs
    chip = lax.rem(me, devs) // 2
    core = lax.rem(me, 2)
    low_half = plane < 2
    outer = (plane == 0) | (plane == PLANES - 1)
    inner = jnp.logical_not(outer)
    beside = jnp.bitwise_xor(plane, 1)
    far = jnp.where(low_half, 3, 0)
    across = jnp.where(low_half, 2, 1)

    mate = jnp.bitwise_xor(me, 1)

    def signal(sem, device):
        pl.semaphore_signal(sem, inc=1, device_id=(device,), device_id_type=MESH)

    beside_core = beside * devs + 2 * chip

    @pl.when(inner & (core == 1))
    def _():
        def greet(k, carry):
            device = devs + k

            @pl.when(device != me)
            def _():
                signal(barrier, device)

            return carry

        lax.fori_loop(0, 2 * devs, greet, 0)
        signal(barrier, beside_core)
        signal(barrier, beside_core + 1)

    @pl.when(outer | (core == 0))
    def _():
        signal(barrier, mate)

    @pl.when(outer)
    def _():
        pl.semaphore_wait(barrier, 2)

    @pl.when(outer & (core == 1))
    def _():
        signal(outer_in, beside_core + 1)

    vregs = state.shape[1]
    quarter = vregs // 4
    bits = vregs.bit_length() - 1
    width = vregs // owners
    full = 8 * n

    loads[0].wait()

    lane = lax.broadcasted_iota(jnp.int32, (8, 128), 1)
    sub = lax.broadcasted_iota(jnp.int32, (8, 128), 0)

    mid = sub_ref[1]
    lane_step = jnp.int32(1)
    for b in range(1, 7):
        lane_step = jnp.where(mid == b, 2**b, lane_step)
    top = 10 + bits - 1
    in_lane = (mid < 7) | (mid == top - 1)
    stride = jnp.int32(vregs // 8)
    for b in range(10, top - 1):
        stride = jnp.where(mid == b, 2 ** (b - 10), stride)
    stride = jnp.where(mid == 7, vregs // 4, stride)
    stride = jnp.where(mid == 9, vregs // 2, stride)
    fixed = mid == 8
    lane_on = jnp.where(in_lane, lane_step, 0)
    lane_hit = jnp.bitwise_and(lane, lane_on) != 0
    lane_keep = lane_hit | (jnp.where(in_lane, 0, 1) != jnp.bitwise_and(lane, 0))
    sub_on = jnp.where(fixed, 0, 2)
    sub_hit = jnp.bitwise_and(sub, sub_on) != 0
    sub_keep = sub_hit | (jnp.where(fixed, 1, 0) != jnp.bitwise_and(sub, 0))

    high4 = sub >= 4
    odd_sub = jnp.bitwise_and(sub, 1) != 0
    odd_lane = jnp.bitwise_and(lane, 1) != 0

    def swap(a, b, hit, keep, step, axis):
        size = (8, 128)[axis]
        back = size - step
        return (
            jnp.where(hit, pltpu.roll(b, step, axis), a),
            jnp.where(keep, b, pltpu.roll(a, back, axis)),
        )

    def spread(c, v):
        x = [state[c, v + quarter * k] for k in range(4)]
        x[0], x[2] = swap(x[0], x[2], high4, high4, 4, 0)
        x[1], x[3] = swap(x[1], x[3], high4, high4, 4, 0)
        for k in (0, 2):
            a, b = swap(x[k], x[k + 1], odd_lane, odd_lane, 1, 1)
            x[k], x[k + 1] = swap(a, b, odd_sub, odd_sub, 1, 0)
        return x

    def fresh(c, at):
        x = spread(c, lax.rem(at, quarter))
        for k in range(3):
            x[3] = jnp.where(at // quarter == k, x[k], x[3])
        return x[3]

    def first_pass(v, carry):
        for c in range(2):
            for k, value in enumerate(spread(c, v)):
                mixed[c, v + quarter * k] = value
        return carry

    pairs = width // 2
    tiles = width // 2
    depth = tiles * 128
    def target(zone, k):
        return zone * chips + jnp.bitwise_xor(chip, chips - 1 - k)

    def pack(owner, read):
        for c in range(2):
            for p in range(pairs):
                u = owner * pairs + p
                low = jnp.bitwise_and(u, stride - 1)
                first = 2 * u - low
                a = read(c, first)
                b = read(c, first + stride)
                a, b = swap(a, b, lane_hit, lane_keep, lane_step, 1)
                a, b = swap(a, b, sub_hit, sub_keep, 2, 0)
                for w, value in enumerate((a, b)):
                    half, tile = divmod(2 * p + w, tiles)
                    column = (c * tiles + tile) * 128
                    send[owner, half, :, column : column + 128] = value

    def pack_group(zone, start):
        def one(k, carry):
            pack(target(zone, k), lambda c, at: mixed[c, at])
            return carry

        lax.fori_loop(start, chips, one, 0, unroll=4 - start if chips >= 4 else 1)

    def send_group(zone, start, stop):
        count = stop - start

        def one(k, carry):
            owner = target(zone, start + lax.rem(k, count))
            half = k // count
            device = 2 * owner + 1

            @pl.when(device != me)
            def _():
                pltpu.make_async_remote_copy(
                    src_ref=send.at[owner, half], dst_ref=recv.at[half, me], send_sem=send_sem,
                    recv_sem=recv_sem.at[plane, half], device_id=(device,), device_id_type=MESH,
                ).start()

            @pl.when(device == me)
            def _():
                pltpu.make_async_copy(
                    send.at[owner, half], recv.at[half, me], recv_sem.at[plane, half]
                ).start()

            return carry

        lax.fori_loop(0, 2 * count, one, 0)

    for load in loads[1:]:
        load.wait()
    pack(target(across, 0), fresh)
    @pl.when(inner)
    def _():
        pl.semaphore_wait(barrier, owners // 2)

    @pl.when(outer)
    def _():
        pl.semaphore_wait(go.at[0], 1)

    @pl.when(outer & (core == 1))
    def _():
        signal(go.at[0], mate)

    send_group(across, 0, 1)

    @pl.when(inner & (core == 1))
    def _():
        pl.semaphore_wait(outer_in, 1)
        signal(go.at[0], beside_core + 1)

        def tell(k, carry):
            device = devs + 2 * k + 1

            @pl.when(device != me)
            def _():
                signal(column_in, device)

            return carry

        lax.fori_loop(0, owners // 2, tell, 0)

    lax.fori_loop(0, quarter, first_pass, 0, unroll=16)
    pack_group(far, 0)

    @pl.when(inner & (core == 1))
    def _():
        pl.semaphore_wait(column_in, owners // 2 - 1)
        signal(go.at[1], mate)
        signal(go.at[1], beside_core + 1)

    @pl.when(outer | (core == 0))
    def _():
        pl.semaphore_wait(go.at[1], 1)

    @pl.when(outer & (core == 1))
    def _():
        signal(go.at[1], mate)

    send_group(far, 0, chips)
    pack_group(beside, 0)
    send_group(beside, 0, chips)
    pack_group(across, 1)
    send_group(across, 1, chips)
    pack_group(plane, 0)
    send_group(plane, 0, chips)

    @pl.when(core == 0)
    def _():
        def tell(k, carry):
            signal(present, 2 * k + 1)
            return carry

        lax.fori_loop(0, owners, tell, 0)


    block = 8 * devs
    wide = max(block, 128)
    ratio = wide // block
    columns = full // 2

    def split(x):
        high = x.astype(jnp.bfloat16)
        return high, (x - high.astype(jnp.float32)).astype(jnp.bfloat16)

    def dot(x, y):
        return lax.dot_general(x, y, (((1,), (1,)), ((), ())), preferred_element_type=jnp.float32)

    def stacked(x):
        return jnp.concatenate(
            [x, jnp.concatenate([x[:, depth:], -x[:, :depth]], axis=1)], axis=0
        )

    def arrival(s):
        second = jnp.where(outer, far, beside)
        third = jnp.where(outer, across, far)
        last = jnp.where(outer, beside, across)
        return jnp.where(
            s == 0, plane, jnp.where(s == 1, second, jnp.where(s == 2, third, last))
        )

    def gram(step, carry):
        crossed = outer & (step >= 4)
        at = jnp.where(crossed, 2 + lax.rem(step, 2), step // 2)
        half = jnp.where(crossed, step // 2 - 2, lax.rem(step, 2))
        zone = arrival(at)
        mine = pl.ds(zone * devs, devs)
        lines = pl.ds(pl.multiple_of(zone * block, block), block)
        came = recv.at[half, mine]
        pltpu.make_async_copy(came, came, recv_sem.at[zone, half]).wait()
        high, low = split(recv[half, mine].reshape(block, 2 * depth))
        high_ref[half, lines] = high
        low_ref[half, lines] = low
        left_h = stacked(high)
        both = dot(jnp.concatenate([left_h, stacked(low)], axis=0), high_ref[half])
        result = both[: 2 * block] + (both[2 * block :] + dot(left_h, low_ref[half]))
        start = lax.rem(zone * block, columns) // wide * wide
        for c in range(2):
            value = result[c * block : (c + 1) * block]
            here = slice(c * columns, (c + 1) * columns)
            for side in range(2):
                piece = value[:, side * columns : (side + 1) * columns]
                part[mine, side, :, here] = part[mine, side, :, here] + piece.reshape(
                    devs, 8, columns
                )
            if c == 1:
                value = -value
            if ratio > 1:
                slot = lax.rem(zone, ratio)
                value = jnp.concatenate(
                    [jnp.where(slot == r, value, 0.0) for r in range(ratio)], axis=0
                )
            turned_ref[c] = value.T.reshape(n, 8, wide)

        def mirror(e, carry):
            there = pl.ds(arrival(e) * devs, devs)
            for c in range(2):
                span = pl.ds(pl.multiple_of(c * columns + start, 128), wide)
                part[there, zone // 2, :, span] = (
                    part[there, zone // 2, :, span] + turned_ref[c, there]
                )
            return carry

        lax.fori_loop(0, at, mirror, 0)
        return carry

    def send_rows(zone, slot, half=None, ready=None, first=0, last=devs):
        def one(k, carry):
            device = zone * devs + k
            if ready is not None:
                ready(device)
            if half is None:
                source, target_rows = part.at[device], rows.at[slot, chip]
            else:
                source, target_rows = part.at[device, half], rows.at[slot, chip, half]

            @pl.when(device != me)
            def _():
                pltpu.make_async_remote_copy(
                    src_ref=source, dst_ref=target_rows, send_sem=row_send,
                    recv_sem=row_recv.at[slot], device_id=(device,), device_id_type=MESH,
                ).start()

            @pl.when(device == me)
            def _():
                pltpu.make_async_copy(source, target_rows, row_recv.at[slot]).start()

            return carry

        lax.fori_loop(first, last, one, 0)

    def add_chain(device):
        part[device] = part[device] + chain[device]

    @pl.when(core == 1)
    def _():
        pl.semaphore_wait(present, owners)
        high_ref[...] = jnp.zeros_like(high_ref)
        low_ref[...] = jnp.zeros_like(low_ref)
        part[...] = jnp.zeros_like(part)
        lax.fori_loop(0, 2 * PLANES - 2, gram, 0)
        near = plane // 2

        @pl.when(inner)
        def _():
            send_rows(beside, 1, near)
            send_rows(plane, 0, near)

        lax.fori_loop(2 * PLANES - 2, 2 * PLANES, gram, 0)

        @pl.when(outer)
        def _():
            for i in range(4):
                mine = pl.ds((far, across)[i // 2] * devs + i % 2 * chips, chips)
                pltpu.make_async_remote_copy(
                    src_ref=part.at[mine], dst_ref=chain.at[mine], send_sem=row_send,
                    recv_sem=chain_sem.at[i], device_id=(beside * devs + 2 * chip + 1,),
                    device_id_type=MESH,
                ).start()
            send_rows(beside, 1)
            send_rows(plane, 0)

        @pl.when(inner)
        def _():
            for i in range(4):
                zone, first = (far, across)[i // 2], i % 2 * chips
                came = chain.at[pl.ds(zone * devs + first, chips)]
                pltpu.make_async_copy(came, came, chain_sem.at[i]).wait()
                if i == 0:
                    pair = min(2, chips)
                    send_rows(zone, 2, ready=add_chain, last=pair)
                    send_rows(beside, 1, 1 - near)
                    first = pair
                send_rows(zone, 2, ready=add_chain, first=first, last=i % 2 * chips + chips)
            send_rows(plane, 0, 1 - near)

    def gathered(slot):
        pltpu.make_async_copy(rows.at[slot], rows.at[slot], row_recv.at[slot]).wait()
        total = rows[slot, 0]
        for k in range(1, chips):
            total = total + rows[slot, k]
        return total

    total = (gathered(0) + gathered(1) + gathered(2)) * scale
    for side in range(2):
        for c in range(2):
            at = c * full + side * columns
            out_ref[:, at : at + columns] = total[side, :, c * columns : (c + 1) * columns]

    rest = send.at[pl.ds(0, owners - 1)]
    pltpu.make_async_copy(rest, rest, send_sem).wait()

    @pl.when(core == 0)
    def _():
        pltpu.make_async_copy(send.at[0], send.at[0], send_sem).wait()

    @pl.when(core == 1)
    def _():
        sent = part.at[pl.ds(0, n - 1)]
        pltpu.make_async_copy(sent, sent, row_send).wait()


def local(n, state_real, state_imag, subsystem):
    amps = state_real.shape[0]
    vregs = amps // 1024
    owners = n // 2
    width = vregs // owners
    full = 8 * n
    devs = n // PLANES
    wide = max(8 * devs, 128)
    chunk = (8, width * 128)
    out = pl.pallas_call(
        functools.partial(exchange_kernel, n, 8.0 / amps),
        out_shape=pltpu.VMEM((8, 2 * full), jnp.float32),
        in_specs=[
            pl.BlockSpec(memory_space=pl.ANY),
            pl.BlockSpec(memory_space=pl.ANY),
            pl.BlockSpec(memory_space=pl.ANY),
        ],
        out_specs=pl.BlockSpec(memory_space=pltpu.VMEM),
        scratch_shapes=[
            pltpu.SMEM((3,), jnp.int32),
            pltpu.VMEM((2, vregs, 8, 128), jnp.float32),
            pltpu.VMEM((2, vregs, 8, 128), jnp.float32),
            pltpu.VMEM((owners, 2) + chunk, jnp.float32),
            pltpu.VMEM((2, n) + chunk, jnp.float32),
            pltpu.VMEM((2, full, chunk[1]), jnp.bfloat16),
            pltpu.VMEM((2, full, chunk[1]), jnp.bfloat16),
            pltpu.VMEM((n, 2, 8, full), jnp.float32),
            pltpu.VMEM((2, n, 8, wide), jnp.float32),
            pltpu.VMEM((n, 2, 8, full), jnp.float32),
            pltpu.VMEM((3, devs // 2, 2, 8, full), jnp.float32),
            pltpu.SemaphoreType.DMA((3,)),
            pltpu.SemaphoreType.DMA,
            pltpu.SemaphoreType.DMA((PLANES, 2)),
            pltpu.SemaphoreType.DMA((4,)),
            pltpu.SemaphoreType.DMA,
            pltpu.SemaphoreType.DMA((3,)),
            pltpu.SemaphoreType.REGULAR,
            pltpu.SemaphoreType.REGULAR,
            pltpu.SemaphoreType.REGULAR,
            pltpu.SemaphoreType.REGULAR((2,)),
        ],
        compiler_params=pltpu.CompilerParams(
            collective_id=0, has_side_effects=True, vmem_limit_bytes=56 * 2**20
        ),
    )(subsystem, state_real.reshape(vregs, 8, 128), state_imag.reshape(vregs, 8, 128))
    return out[:, :full], out[:, full:]


def solution(mesh):
    return jax.shard_map(
        functools.partial(local, mesh.shape["dev"]),
        mesh=mesh,
        in_specs=(P("dev"), P("dev"), P()),
        out_specs=(P("dev", None), P("dev", None)),
        check_vma=False,
    )
```

```python
import functools

import jax
import jax.numpy as jnp
from jax import lax
from jax.experimental import pallas as pl
from jax.experimental.pallas import tpu as pltpu
from jax.sharding import PartitionSpec as P

MESH = pl.DeviceIdType.MESH
PLANES = 4


def piece_tiles(width):
    last = max(1, width // 4)
    return width - last, last


def exchange_kernel(n, scale, sub_hbm, re_hbm, im_hbm, out_ref, sub_ref, state, mixed, send_a,
                    send_b, recv_a, recv_b, high_a, high_b, low_a, low_b, part, turned_ref, chain, rows, load_sem, send_sem,
                    recv_sem, chain_sem, row_send, row_recv, present, outer_in, column_in, go):
    me = lax.axis_index("dev")
    loads = [
        pltpu.make_async_copy(sub_hbm, sub_ref, load_sem.at[2]),
        pltpu.make_async_copy(re_hbm, state.at[0], load_sem.at[0]),
        pltpu.make_async_copy(im_hbm, state.at[1], load_sem.at[1]),
    ]
    for load in loads:
        load.start()
    barrier = pltpu.get_barrier_semaphore()

    devs = n // PLANES
    chips = devs // 2
    owners = n // 2
    plane = me // devs
    chip = lax.rem(me, devs) // 2
    core = lax.rem(me, 2)
    low_half = plane < 2
    outer = (plane == 0) | (plane == PLANES - 1)
    inner = jnp.logical_not(outer)
    beside = jnp.bitwise_xor(plane, 1)
    far = jnp.where(low_half, 3, 0)
    across = jnp.where(low_half, 2, 1)

    mate = jnp.bitwise_xor(me, 1)

    def signal(sem, device):
        pl.semaphore_signal(sem, inc=1, device_id=(device,), device_id_type=MESH)

    beside_core = beside * devs + 2 * chip

    @pl.when(inner & (core == 1))
    def _():
        def greet(k, carry):
            device = devs + k

            @pl.when(device != me)
            def _():
                signal(barrier, device)

            return carry

        lax.fori_loop(0, 2 * devs, greet, 0)
        signal(barrier, beside_core)
        signal(barrier, beside_core + 1)

    @pl.when(outer | (core == 0))
    def _():
        signal(barrier, mate)

    @pl.when(outer)
    def _():
        pl.semaphore_wait(barrier, 2)

    @pl.when(outer & (core == 1))
    def _():
        signal(outer_in, beside_core + 1)

    vregs = state.shape[1]
    quarter = vregs // 4
    bits = vregs.bit_length() - 1
    width = vregs // owners
    full = 8 * n

    loads[0].wait()

    lane = lax.broadcasted_iota(jnp.int32, (8, 128), 1)
    sub = lax.broadcasted_iota(jnp.int32, (8, 128), 0)

    mid = sub_ref[1]
    lane_step = jnp.int32(1)
    for b in range(1, 7):
        lane_step = jnp.where(mid == b, 2**b, lane_step)
    top = 10 + bits - 1
    in_lane = (mid < 7) | (mid == top - 1)
    stride = jnp.int32(vregs // 8)
    for b in range(10, top - 1):
        stride = jnp.where(mid == b, 2 ** (b - 10), stride)
    stride = jnp.where(mid == 7, vregs // 4, stride)
    stride = jnp.where(mid == 9, vregs // 2, stride)
    fixed = mid == 8
    lane_on = jnp.where(in_lane, lane_step, 0)
    lane_hit = jnp.bitwise_and(lane, lane_on) != 0
    lane_keep = lane_hit | (jnp.where(in_lane, 0, 1) != jnp.bitwise_and(lane, 0))
    sub_on = jnp.where(fixed, 0, 2)
    sub_hit = jnp.bitwise_and(sub, sub_on) != 0
    sub_keep = sub_hit | (jnp.where(fixed, 1, 0) != jnp.bitwise_and(sub, 0))

    high4 = sub >= 4
    odd_sub = jnp.bitwise_and(sub, 1) != 0
    odd_lane = jnp.bitwise_and(lane, 1) != 0

    def swap(a, b, hit, keep, step, axis):
        size = (8, 128)[axis]
        back = size - step
        return (
            jnp.where(hit, pltpu.roll(b, step, axis), a),
            jnp.where(keep, b, pltpu.roll(a, back, axis)),
        )

    def spread(c, v):
        x = [state[c, v + quarter * k] for k in range(4)]
        x[0], x[2] = swap(x[0], x[2], high4, high4, 4, 0)
        x[1], x[3] = swap(x[1], x[3], high4, high4, 4, 0)
        for k in (0, 2):
            a, b = swap(x[k], x[k + 1], odd_lane, odd_lane, 1, 1)
            x[k], x[k + 1] = swap(a, b, odd_sub, odd_sub, 1, 0)
        return x

    def fresh(c, at):
        x = spread(c, lax.rem(at, quarter))
        for k in range(3):
            x[3] = jnp.where(at // quarter == k, x[k], x[3])
        return x[3]

    def first_pass(v, carry):
        for c in range(2):
            for k, value in enumerate(spread(c, v)):
                mixed[c, v + quarter * k] = value
        return carry

    pairs = width // 2
    send, recv = (send_a, send_b), (recv_a, recv_b)
    high_ref, low_ref = (high_a, high_b), (low_a, low_b)
    tiles = piece_tiles(width)
    def target(zone, k):
        return zone * chips + jnp.bitwise_xor(chip, chips - 1 - k)

    def pack(owner, read):
        for c in range(2):
            for p in range(pairs):
                u = owner * pairs + p
                low = jnp.bitwise_and(u, stride - 1)
                first = 2 * u - low
                a = read(c, first)
                b = read(c, first + stride)
                a, b = swap(a, b, lane_hit, lane_keep, lane_step, 1)
                a, b = swap(a, b, sub_hit, sub_keep, 2, 0)
                for w, value in enumerate((a, b)):
                    tile = 2 * p + w
                    piece = int(tile >= tiles[0])
                    column = (c * tiles[piece] + tile - piece * tiles[0]) * 128
                    send[piece][owner, :, column : column + 128] = value

    def pack_group(zone, start):
        def one(k, carry):
            pack(target(zone, k), lambda c, at: mixed[c, at])
            return carry

        lax.fori_loop(start, chips, one, 0, unroll=4 - start if chips >= 4 else 1)

    def send_group(zone, start, stop):
        for piece in range(2):
            def one(k, carry):
                owner = target(zone, k)
                device = 2 * owner + 1
                arrived = recv_sem.at[plane, piece]
                source, there = send[piece].at[owner], recv[piece].at[me]

                @pl.when(device != me)
                def _():
                    pltpu.make_async_remote_copy(
                        src_ref=source, dst_ref=there, send_sem=send_sem, recv_sem=arrived,
                        device_id=(device,), device_id_type=MESH,
                    ).start()

                @pl.when(device == me)
                def _():
                    pltpu.make_async_copy(source, there, arrived).start()

                return carry

            lax.fori_loop(start, stop, one, 0)

    for load in loads[1:]:
        load.wait()
    pack(target(across, 0), fresh)
    @pl.when(inner)
    def _():
        pl.semaphore_wait(barrier, owners // 2)

    @pl.when(outer)
    def _():
        pl.semaphore_wait(go.at[0], 1)

    @pl.when(outer & (core == 1))
    def _():
        signal(go.at[0], mate)

    send_group(across, 0, 1)

    @pl.when(inner & (core == 1))
    def _():
        pl.semaphore_wait(outer_in, 1)
        signal(go.at[0], beside_core + 1)

        def tell(k, carry):
            device = devs + 2 * k + 1

            @pl.when(device != me)
            def _():
                signal(column_in, device)

            return carry

        lax.fori_loop(0, owners // 2, tell, 0)

    lax.fori_loop(0, quarter, first_pass, 0, unroll=16)
    pack_group(far, 0)

    @pl.when(inner & (core == 1))
    def _():
        pl.semaphore_wait(column_in, owners // 2 - 1)
        signal(go.at[1], mate)
        signal(go.at[1], beside_core + 1)

    @pl.when(outer | (core == 0))
    def _():
        pl.semaphore_wait(go.at[1], 1)

    @pl.when(outer & (core == 1))
    def _():
        signal(go.at[1], mate)

    send_group(far, 0, chips)
    pack_group(beside, 0)
    send_group(beside, 0, chips)
    pack_group(across, 1)
    send_group(across, 1, chips)
    pack_group(plane, 0)
    send_group(plane, 0, chips)

    @pl.when(core == 0)
    def _():
        def tell(k, carry):
            signal(present, 2 * k + 1)
            return carry

        lax.fori_loop(0, owners, tell, 0)


    block = 8 * devs
    wide = max(block, 128)
    ratio = wide // block
    columns = full // 2

    def split(x):
        high = x.astype(jnp.bfloat16)
        return high, (x - high.astype(jnp.float32)).astype(jnp.bfloat16)

    def dot(x, y):
        return lax.dot_general(x, y, (((1,), (1,)), ((), ())), preferred_element_type=jnp.float32)

    def stacked(x):
        depth = x.shape[1] // 2
        return jnp.concatenate(
            [x, jnp.concatenate([x[:, depth:], -x[:, :depth]], axis=1)], axis=0
        )

    def arrival(s):
        second = jnp.where(outer, far, beside)
        third = jnp.where(outer, across, far)
        last = jnp.where(outer, beside, across)
        return jnp.where(
            s == 0, plane, jnp.where(s == 1, second, jnp.where(s == 2, third, last))
        )

    def gram(at, piece):
        zone = arrival(at)
        mine = pl.ds(zone * devs, devs)
        lines = pl.ds(pl.multiple_of(zone * block, block), block)
        came = recv[piece].at[mine]
        pltpu.make_async_copy(came, came, recv_sem.at[zone, piece]).wait()
        high, low = split(recv[piece][mine].reshape(block, 256 * tiles[piece]))
        high_ref[piece][lines] = high
        low_ref[piece][lines] = low
        left_h = stacked(high)
        both = dot(jnp.concatenate([left_h, stacked(low)], axis=0), high_ref[piece][...])
        result = both[: 2 * block] + (both[2 * block :] + dot(left_h, low_ref[piece][...]))
        start = lax.rem(zone * block, columns) // wide * wide
        for c in range(2):
            value = result[c * block : (c + 1) * block]
            here = slice(c * columns, (c + 1) * columns)
            for side in range(2):
                added = value[:, side * columns : (side + 1) * columns]
                part[mine, side, :, here] = part[mine, side, :, here] + added.reshape(
                    devs, 8, columns
                )
            if c == 1:
                value = -value
            if ratio > 1:
                slot = lax.rem(zone, ratio)
                value = jnp.concatenate(
                    [jnp.where(slot == r, value, 0.0) for r in range(ratio)], axis=0
                )
            turned_ref[c] = value.T.reshape(n, 8, wide)

        def mirror(e, carry):
            there = pl.ds(arrival(e) * devs, devs)
            for c in range(2):
                span = pl.ds(pl.multiple_of(c * columns + start, 128), wide)
                part[there, zone // 2, :, span] = (
                    part[there, zone // 2, :, span] + turned_ref[c, there]
                )
            return carry

        lax.fori_loop(0, at, mirror, 0)

    def send_rows(zone, slot, half=None, ready=None, first=0, last=devs):
        def one(k, carry):
            device = zone * devs + k
            if ready is not None:
                ready(device)
            if half is None:
                source, target_rows = part.at[device], rows.at[slot, chip]
            else:
                source, target_rows = part.at[device, half], rows.at[slot, chip, half]

            @pl.when(device != me)
            def _():
                pltpu.make_async_remote_copy(
                    src_ref=source, dst_ref=target_rows, send_sem=row_send,
                    recv_sem=row_recv.at[slot], device_id=(device,), device_id_type=MESH,
                ).start()

            @pl.when(device == me)
            def _():
                pltpu.make_async_copy(source, target_rows, row_recv.at[slot]).start()

            return carry

        lax.fori_loop(first, last, one, 0)

    def add_chain(device):
        part[device] = part[device] + chain[device]

    @pl.when(core == 1)
    def _():
        pl.semaphore_wait(present, owners)
        for ref in (*high_ref, *low_ref, part):
            ref[...] = jnp.zeros_like(ref)

        near = plane // 2

        def step(i, carry):
            crossed = outer & (i >= 4)
            at = jnp.where(crossed, 2 + lax.rem(i, 2), i // 2)
            piece = jnp.where(crossed, i // 2 - 2, lax.rem(i, 2))
            for p in range(2):
                pl.when(piece == p)(functools.partial(gram, at, p))

            @pl.when(inner & ((i == 5) | (i == 7)))
            def _():
                send_rows(beside, 1, jnp.where(i == 5, near, 1 - near))

            return carry

        lax.fori_loop(0, 2 * PLANES, step, 0)

        @pl.when(outer)
        def _():
            for i in range(4):
                mine = pl.ds((far, across)[i // 2] * devs + i % 2 * chips, chips)
                pltpu.make_async_remote_copy(
                    src_ref=part.at[mine], dst_ref=chain.at[mine], send_sem=row_send,
                    recv_sem=chain_sem.at[i], device_id=(beside * devs + 2 * chip + 1,),
                    device_id_type=MESH,
                ).start()
            send_rows(beside, 1)
            send_rows(plane, 0)

        @pl.when(inner)
        def _():
            def relay(i, carry):
                zone, first = jnp.where(i < 2, far, across), lax.rem(i, 2) * chips
                came = chain.at[pl.ds(zone * devs + first, chips)]
                pltpu.make_async_copy(came, came, chain_sem.at[i]).wait()
                send_rows(zone, 2, ready=add_chain, first=first, last=first + chips)
                return carry

            lax.fori_loop(0, 4, relay, 0)
            send_rows(plane, 0)

    def gathered(slot):
        pltpu.make_async_copy(rows.at[slot], rows.at[slot], row_recv.at[slot]).wait()
        total = rows[slot, 0]
        for k in range(1, chips):
            total = total + rows[slot, k]
        return total

    total = (gathered(0) + gathered(1) + gathered(2)) * scale
    for side in range(2):
        for c in range(2):
            at = c * full + side * columns
            out_ref[:, at : at + columns] = total[side, :, c * columns : (c + 1) * columns]

    for ref in send:
        rest = ref.at[pl.ds(0, owners - 1)]
        pltpu.make_async_copy(rest, rest, send_sem).wait()

    @pl.when(core == 0)
    def _():
        for ref in send:
            pltpu.make_async_copy(ref.at[0], ref.at[0], send_sem).wait()

    @pl.when(core == 1)
    def _():
        sent = part.at[pl.ds(0, n - 1)]
        pltpu.make_async_copy(sent, sent, row_send).wait()


def local(n, state_real, state_imag, subsystem):
    amps = state_real.shape[0]
    vregs = amps // 1024
    owners = n // 2
    width = vregs // owners
    full = 8 * n
    devs = n // PLANES
    wide = max(8 * devs, 128)
    depths = [256 * tiles for tiles in piece_tiles(width)]
    out = pl.pallas_call(
        functools.partial(exchange_kernel, n, 8.0 / amps),
        out_shape=pltpu.VMEM((8, 2 * full), jnp.float32),
        in_specs=[
            pl.BlockSpec(memory_space=pl.ANY),
            pl.BlockSpec(memory_space=pl.ANY),
            pl.BlockSpec(memory_space=pl.ANY),
        ],
        out_specs=pl.BlockSpec(memory_space=pltpu.VMEM),
        scratch_shapes=[
            pltpu.SMEM((3,), jnp.int32),
            pltpu.VMEM((2, vregs, 8, 128), jnp.float32),
            pltpu.VMEM((2, vregs, 8, 128), jnp.float32),
            *[pltpu.VMEM((owners, 8, depth), jnp.float32) for depth in depths],
            *[pltpu.VMEM((n, 8, depth), jnp.float32) for depth in depths],
            *[pltpu.VMEM((full, depth), jnp.bfloat16) for depth in depths],
            *[pltpu.VMEM((full, depth), jnp.bfloat16) for depth in depths],
            pltpu.VMEM((n, 2, 8, full), jnp.float32),
            pltpu.VMEM((2, n, 8, wide), jnp.float32),
            pltpu.VMEM((n, 2, 8, full), jnp.float32),
            pltpu.VMEM((3, devs // 2, 2, 8, full), jnp.float32),
            pltpu.SemaphoreType.DMA((3,)),
            pltpu.SemaphoreType.DMA,
            pltpu.SemaphoreType.DMA((PLANES, 2)),
            pltpu.SemaphoreType.DMA((4,)),
            pltpu.SemaphoreType.DMA,
            pltpu.SemaphoreType.DMA((3,)),
            pltpu.SemaphoreType.REGULAR,
            pltpu.SemaphoreType.REGULAR,
            pltpu.SemaphoreType.REGULAR,
            pltpu.SemaphoreType.REGULAR((2,)),
        ],
        compiler_params=pltpu.CompilerParams(
            collective_id=0, has_side_effects=True, vmem_limit_bytes=56 * 2**20
        ),
    )(subsystem, state_real.reshape(vregs, 8, 128), state_imag.reshape(vregs, 8, 128))
    return out[:, :full], out[:, full:]


def solution(mesh):
    return jax.shard_map(
        functools.partial(local, mesh.shape["dev"]),
        mesh=mesh,
        in_specs=(P("dev"), P("dev"), P()),
        out_specs=(P("dev", None), P("dev", None)),
        check_vma=False,
    )
```

```python
import functools

import jax
import jax.numpy as jnp
from jax import lax
from jax.experimental import pallas as pl
from jax.experimental.pallas import tpu as pltpu
from jax.sharding import PartitionSpec as P

MESH = pl.DeviceIdType.MESH
PLANES = 4


def piece_tiles(width):
    last = max(1, width // 4)
    return width - last, last


def exchange_kernel(n, scale, sub_hbm, re_hbm, im_hbm, out_ref, sub_ref, state, mixed, send_a,
                    send_b, recv_a, recv_b, high_a, high_b, low_a, low_b, part, turned_ref, chain, rows, load_sem, send_sem,
                    recv_sem, chain_sem, row_send, row_recv, present, outer_in, column_in, go):
    me = lax.axis_index("dev")
    loads = [
        pltpu.make_async_copy(sub_hbm, sub_ref, load_sem.at[2]),
        pltpu.make_async_copy(re_hbm, state.at[0], load_sem.at[0]),
        pltpu.make_async_copy(im_hbm, state.at[1], load_sem.at[1]),
    ]
    for load in loads:
        load.start()
    barrier = pltpu.get_barrier_semaphore()

    devs = n // PLANES
    chips = devs // 2
    owners = n // 2
    plane = me // devs
    chip = lax.rem(me, devs) // 2
    core = lax.rem(me, 2)
    low_half = plane < 2
    outer = (plane == 0) | (plane == PLANES - 1)
    inner = jnp.logical_not(outer)
    beside = jnp.bitwise_xor(plane, 1)
    far = jnp.where(low_half, 3, 0)
    across = jnp.where(low_half, 2, 1)

    mate = jnp.bitwise_xor(me, 1)

    def signal(sem, device):
        pl.semaphore_signal(sem, inc=1, device_id=(device,), device_id_type=MESH)

    beside_core = beside * devs + 2 * chip

    @pl.when(inner & (core == 1))
    def _():
        def greet(k, carry):
            device = devs + k

            @pl.when(device != me)
            def _():
                signal(barrier, device)

            return carry

        lax.fori_loop(0, 2 * devs, greet, 0)
        signal(barrier, beside_core)
        signal(barrier, beside_core + 1)

    @pl.when(outer | (core == 0))
    def _():
        signal(barrier, mate)

    @pl.when(outer)
    def _():
        pl.semaphore_wait(barrier, 2)

    @pl.when(outer & (core == 1))
    def _():
        signal(outer_in, beside_core + 1)

    vregs = state.shape[1]
    quarter = vregs // 4
    bits = vregs.bit_length() - 1
    width = vregs // owners
    full = 8 * n

    loads[0].wait()

    lane = lax.broadcasted_iota(jnp.int32, (8, 128), 1)
    sub = lax.broadcasted_iota(jnp.int32, (8, 128), 0)

    mid = sub_ref[1]
    lane_step = jnp.int32(1)
    for b in range(1, 7):
        lane_step = jnp.where(mid == b, 2**b, lane_step)
    top = 10 + bits - 1
    in_lane = (mid < 7) | (mid == top - 1)
    stride = jnp.int32(vregs // 8)
    for b in range(10, top - 1):
        stride = jnp.where(mid == b, 2 ** (b - 10), stride)
    stride = jnp.where(mid == 7, vregs // 4, stride)
    stride = jnp.where(mid == 9, vregs // 2, stride)
    fixed = mid == 8
    lane_on = jnp.where(in_lane, lane_step, 0)
    lane_hit = jnp.bitwise_and(lane, lane_on) != 0
    lane_keep = lane_hit | (jnp.where(in_lane, 0, 1) != jnp.bitwise_and(lane, 0))
    sub_on = jnp.where(fixed, 0, 2)
    sub_hit = jnp.bitwise_and(sub, sub_on) != 0
    sub_keep = sub_hit | (jnp.where(fixed, 1, 0) != jnp.bitwise_and(sub, 0))

    high4 = sub >= 4
    odd_sub = jnp.bitwise_and(sub, 1) != 0
    odd_lane = jnp.bitwise_and(lane, 1) != 0

    def swap(a, b, hit, keep, step, axis):
        size = (8, 128)[axis]
        back = size - step
        return (
            jnp.where(hit, pltpu.roll(b, step, axis), a),
            jnp.where(keep, b, pltpu.roll(a, back, axis)),
        )

    def spread(c, v):
        x = [state[c, v + quarter * k] for k in range(4)]
        x[0], x[2] = swap(x[0], x[2], high4, high4, 4, 0)
        x[1], x[3] = swap(x[1], x[3], high4, high4, 4, 0)
        for k in (0, 2):
            a, b = swap(x[k], x[k + 1], odd_lane, odd_lane, 1, 1)
            x[k], x[k + 1] = swap(a, b, odd_sub, odd_sub, 1, 0)
        return x

    def fresh(c, at):
        x = spread(c, lax.rem(at, quarter))
        for k in range(3):
            x[3] = jnp.where(at // quarter == k, x[k], x[3])
        return x[3]

    def first_pass(v, carry):
        for c in range(2):
            for k, value in enumerate(spread(c, v)):
                mixed[c, v + quarter * k] = value
        return carry

    pairs = width // 2
    send, recv = (send_a, send_b), (recv_a, recv_b)
    high_ref, low_ref = (high_a, high_b), (low_a, low_b)
    tiles = piece_tiles(width)
    def target(zone, k):
        return zone * chips + jnp.bitwise_xor(chip, chips - 1 - k)

    def pack(owner, read):
        for c in range(2):
            for p in range(pairs):
                u = owner * pairs + p
                low = jnp.bitwise_and(u, stride - 1)
                first = 2 * u - low
                a = read(c, first)
                b = read(c, first + stride)
                a, b = swap(a, b, lane_hit, lane_keep, lane_step, 1)
                a, b = swap(a, b, sub_hit, sub_keep, 2, 0)
                for w, value in enumerate((a, b)):
                    tile = 2 * p + w
                    piece = int(tile >= tiles[0])
                    column = (c * tiles[piece] + tile - piece * tiles[0]) * 128
                    send[piece][owner, :, column : column + 128] = value

    def pack_group(zone, start):
        def one(k, carry):
            pack(target(zone, k), lambda c, at: mixed[c, at])
            return carry

        lax.fori_loop(start, chips, one, 0, unroll=4 - start if chips >= 4 else 1)

    def send_group(zone, start, stop):
        for piece in range(2):
            def one(k, carry):
                owner = target(zone, k)
                device = 2 * owner + 1
                arrived = recv_sem.at[plane, piece]
                source, there = send[piece].at[owner], recv[piece].at[me]

                @pl.when(device != me)
                def _():
                    pltpu.make_async_remote_copy(
                        src_ref=source, dst_ref=there, send_sem=send_sem, recv_sem=arrived,
                        device_id=(device,), device_id_type=MESH,
                    ).start()

                @pl.when(device == me)
                def _():
                    pltpu.make_async_copy(source, there, arrived).start()

                return carry

            lax.fori_loop(start, stop, one, 0)

    for load in loads[1:]:
        load.wait()
    pack(target(across, 0), fresh)
    @pl.when(inner)
    def _():
        pl.semaphore_wait(barrier, owners // 2)

    @pl.when(outer)
    def _():
        pl.semaphore_wait(go.at[0], 1)

    @pl.when(outer & (core == 1))
    def _():
        signal(go.at[0], mate)

    send_group(across, 0, 1)

    @pl.when(inner & (core == 1))
    def _():
        pl.semaphore_wait(outer_in, 1)
        signal(go.at[0], beside_core + 1)

        def tell(k, carry):
            device = devs + 2 * k + 1

            @pl.when(device != me)
            def _():
                signal(column_in, device)

            return carry

        lax.fori_loop(0, owners // 2, tell, 0)

    lax.fori_loop(0, quarter, first_pass, 0, unroll=16)
    pack_group(far, 0)

    @pl.when(inner & (core == 1))
    def _():
        pl.semaphore_wait(column_in, owners // 2 - 1)
        signal(go.at[1], mate)
        signal(go.at[1], beside_core + 1)

    @pl.when(outer | (core == 0))
    def _():
        pl.semaphore_wait(go.at[1], 1)

    @pl.when(outer & (core == 1))
    def _():
        signal(go.at[1], mate)

    send_group(far, 0, chips)
    pack_group(beside, 0)
    send_group(beside, 0, chips)
    pack_group(across, 1)
    send_group(across, 1, chips)
    pack_group(plane, 0)
    send_group(plane, 0, chips)

    @pl.when(core == 0)
    def _():
        def tell(k, carry):
            signal(present, 2 * k + 1)
            return carry

        lax.fori_loop(0, owners, tell, 0)


    block = 8 * devs
    wide = max(block, 128)
    ratio = wide // block
    columns = full // 2

    def split(x):
        high = x.astype(jnp.bfloat16)
        return high, (x - high.astype(jnp.float32)).astype(jnp.bfloat16)

    def dot(x, y):
        return lax.dot_general(x, y, (((1,), (1,)), ((), ())), preferred_element_type=jnp.float32)

    def stacked(x):
        depth = x.shape[1] // 2
        return jnp.concatenate(
            [x, jnp.concatenate([x[:, depth:], -x[:, :depth]], axis=1)], axis=0
        )

    def arrival(s):
        second = jnp.where(outer, far, beside)
        third = jnp.where(outer, across, far)
        last = jnp.where(outer, beside, across)
        return jnp.where(
            s == 0, plane, jnp.where(s == 1, second, jnp.where(s == 2, third, last))
        )

    def gram(at, piece):
        zone = arrival(at)
        mine = pl.ds(zone * devs, devs)
        lines = pl.ds(pl.multiple_of(zone * block, block), block)
        came = recv[piece].at[mine]
        pltpu.make_async_copy(came, came, recv_sem.at[zone, piece]).wait()
        high, low = split(recv[piece][mine].reshape(block, 256 * tiles[piece]))
        high_ref[piece][lines] = high
        low_ref[piece][lines] = low
        left_h = stacked(high)
        both = dot(jnp.concatenate([left_h, stacked(low)], axis=0), high_ref[piece][...])
        result = both[: 2 * block] + (both[2 * block :] + dot(left_h, low_ref[piece][...]))
        start = lax.rem(zone * block, columns) // wide * wide
        for c in range(2):
            value = result[c * block : (c + 1) * block]
            here = slice(c * columns, (c + 1) * columns)
            for side in range(2):
                added = value[:, side * columns : (side + 1) * columns]
                part[mine, side, :, here] = part[mine, side, :, here] + added.reshape(
                    devs, 8, columns
                )
            if c == 1:
                value = -value
            if ratio > 1:
                slot = lax.rem(zone, ratio)
                value = jnp.concatenate(
                    [jnp.where(slot == r, value, 0.0) for r in range(ratio)], axis=0
                )
            turned_ref[c] = value.T.reshape(n, 8, wide)

        def mirror(e, carry):
            there = pl.ds(arrival(e) * devs, devs)
            for c in range(2):
                span = pl.ds(pl.multiple_of(c * columns + start, 128), wide)
                part[there, zone // 2, :, span] = (
                    part[there, zone // 2, :, span] + turned_ref[c, there]
                )
            return carry

        lax.fori_loop(0, at, mirror, 0)

    def send_rows(zone, slot, half=None, ready=None, first=0, last=devs):
        def one(k, carry):
            device = zone * devs + k
            if ready is not None:
                ready(device)
            if half is None:
                source, target_rows = part.at[device], rows.at[slot, chip]
            else:
                source, target_rows = part.at[device, half], rows.at[slot, chip, half]

            @pl.when(device != me)
            def _():
                pltpu.make_async_remote_copy(
                    src_ref=source, dst_ref=target_rows, send_sem=row_send,
                    recv_sem=row_recv.at[slot], device_id=(device,), device_id_type=MESH,
                ).start()

            @pl.when(device == me)
            def _():
                pltpu.make_async_copy(source, target_rows, row_recv.at[slot]).start()

            return carry

        lax.fori_loop(first, last, one, 0)

    def add_chain(device):
        part[device] = part[device] + chain[device]

    @pl.when(core == 1)
    def _():
        pl.semaphore_wait(present, owners)
        for ref in (*high_ref, *low_ref, part):
            ref[...] = jnp.zeros_like(ref)

        near = plane // 2

        def step(i, carry):
            crossed = outer & (i >= 4)
            at = jnp.where(crossed, 2 + lax.rem(i, 2), i // 2)
            piece = jnp.where(crossed, i // 2 - 2, lax.rem(i, 2))
            for p in range(2):
                pl.when(piece == p)(functools.partial(gram, at, p))

            @pl.when(inner & ((i == 5) | (i == 7)))
            def _():
                send_rows(beside, 1, jnp.where(i == 5, near, 1 - near))

            return carry

        lax.fori_loop(0, 2 * PLANES, step, 0)

        @pl.when(outer)
        def _():
            for i in range(4):
                mine = pl.ds((far, across)[i // 2] * devs + i % 2 * chips, chips)
                pltpu.make_async_remote_copy(
                    src_ref=part.at[mine], dst_ref=chain.at[mine], send_sem=row_send,
                    recv_sem=chain_sem.at[i], device_id=(beside * devs + 2 * chip + 1,),
                    device_id_type=MESH,
                ).start()
            send_rows(beside, 1)
            send_rows(plane, 0)

        @pl.when(inner)
        def _():
            def relay(i, carry):
                zone, first = jnp.where(i < 2, far, across), lax.rem(i, 2) * chips
                came = chain.at[pl.ds(zone * devs + first, chips)]
                pltpu.make_async_copy(came, came, chain_sem.at[i]).wait()
                send_rows(zone, 2, ready=add_chain, first=first, last=first + chips)
                return carry

            lax.fori_loop(0, 4, relay, 0)
            send_rows(plane, 0)

    for ref in send:
        rest = ref.at[pl.ds(0, owners - 1)]
        pltpu.make_async_copy(rest, rest, send_sem).wait()

    @pl.when(core == 0)
    def _():
        for ref in send:
            pltpu.make_async_copy(ref.at[0], ref.at[0], send_sem).wait()

    @pl.when(core == 1)
    def _():
        sent = part.at[pl.ds(0, n - 1)]
        pltpu.make_async_copy(sent, sent, row_send).wait()

    def gather(slot, total):
        came = rows.at[slot]
        pltpu.make_async_copy(came, came, row_recv.at[slot]).wait()
        for k in range(chips):
            total = total + rows[slot, k]
        return total

    total = lax.fori_loop(0, 3, gather, jnp.zeros((2, 8, full), jnp.float32)) * scale
    for side in range(2):
        for c in range(2):
            at = c * full + side * columns
            out_ref[:, at : at + columns] = total[side, :, c * columns : (c + 1) * columns]


def local(n, state_real, state_imag, subsystem):
    amps = state_real.shape[0]
    vregs = amps // 1024
    owners = n // 2
    width = vregs // owners
    full = 8 * n
    devs = n // PLANES
    wide = max(8 * devs, 128)
    depths = [256 * tiles for tiles in piece_tiles(width)]
    out = pl.pallas_call(
        functools.partial(exchange_kernel, n, 8.0 / amps),
        out_shape=pltpu.VMEM((8, 2 * full), jnp.float32),
        in_specs=[
            pl.BlockSpec(memory_space=pl.ANY),
            pl.BlockSpec(memory_space=pl.ANY),
            pl.BlockSpec(memory_space=pl.ANY),
        ],
        out_specs=pl.BlockSpec(memory_space=pltpu.VMEM),
        scratch_shapes=[
            pltpu.SMEM((3,), jnp.int32),
            pltpu.VMEM((2, vregs, 8, 128), jnp.float32),
            pltpu.VMEM((2, vregs, 8, 128), jnp.float32),
            *[pltpu.VMEM((owners, 8, depth), jnp.float32) for depth in depths],
            *[pltpu.VMEM((n, 8, depth), jnp.float32) for depth in depths],
            *[pltpu.VMEM((full, depth), jnp.bfloat16) for depth in depths],
            *[pltpu.VMEM((full, depth), jnp.bfloat16) for depth in depths],
            pltpu.VMEM((n, 2, 8, full), jnp.float32),
            pltpu.VMEM((2, n, 8, wide), jnp.float32),
            pltpu.VMEM((n, 2, 8, full), jnp.float32),
            pltpu.VMEM((3, devs // 2, 2, 8, full), jnp.float32),
            pltpu.SemaphoreType.DMA((3,)),
            pltpu.SemaphoreType.DMA,
            pltpu.SemaphoreType.DMA((PLANES, 2)),
            pltpu.SemaphoreType.DMA((4,)),
            pltpu.SemaphoreType.DMA,
            pltpu.SemaphoreType.DMA((3,)),
            pltpu.SemaphoreType.REGULAR,
            pltpu.SemaphoreType.REGULAR,
            pltpu.SemaphoreType.REGULAR,
            pltpu.SemaphoreType.REGULAR((2,)),
        ],
        compiler_params=pltpu.CompilerParams(
            collective_id=0, has_side_effects=True, vmem_limit_bytes=56 * 2**20
        ),
    )(subsystem, state_real.reshape(vregs, 8, 128), state_imag.reshape(vregs, 8, 128))
    return out[:, :full], out[:, full:]


def solution(mesh):
    return jax.shard_map(
        functools.partial(local, mesh.shape["dev"]),
        mesh=mesh,
        in_specs=(P("dev"), P("dev"), P()),
        out_specs=(P("dev", None), P("dev", None)),
        check_vma=False,
    )
```

```python
import functools

import jax
import jax.numpy as jnp
from jax import lax
from jax.experimental import pallas as pl
from jax.experimental.pallas import tpu as pltpu
from jax.sharding import PartitionSpec as P

MESH = pl.DeviceIdType.MESH
PLANES = 4


def piece_tiles(width):
    last = max(1, width // 4)
    return width - last, last


def exchange_kernel(n, scale, sub_hbm, re_hbm, im_hbm, out_ref, sub_ref, state, mixed, send_a,
                    send_b, recv_a, recv_b, high_a, high_b, low_a, low_b, part, turned_ref, chain, rows, load_sem, send_sem,
                    recv_sem, chain_sem, row_send, row_recv, present, outer_in, column_in, go):
    me = lax.axis_index("dev")
    loads = [
        pltpu.make_async_copy(sub_hbm, sub_ref, load_sem.at[2]),
        pltpu.make_async_copy(re_hbm, state.at[0], load_sem.at[0]),
        pltpu.make_async_copy(im_hbm, state.at[1], load_sem.at[1]),
    ]
    for load in loads:
        load.start()
    barrier = pltpu.get_barrier_semaphore()

    devs = n // PLANES
    chips = devs // 2
    owners = n // 2
    plane = me // devs
    chip = lax.rem(me, devs) // 2
    core = lax.rem(me, 2)
    low_half = plane < 2
    outer = (plane == 0) | (plane == PLANES - 1)
    inner = jnp.logical_not(outer)
    beside = jnp.bitwise_xor(plane, 1)
    far = jnp.where(low_half, 3, 0)
    across = jnp.where(low_half, 2, 1)

    mate = jnp.bitwise_xor(me, 1)

    def signal(sem, device):
        pl.semaphore_signal(sem, inc=1, device_id=(device,), device_id_type=MESH)

    beside_core = beside * devs + 2 * chip

    @pl.when(inner & (core == 1))
    def _():
        def greet(k, carry):
            device = devs + k

            @pl.when(device != me)
            def _():
                signal(barrier, device)

            return carry

        lax.fori_loop(0, 2 * devs, greet, 0)
        signal(barrier, beside_core)
        signal(barrier, beside_core + 1)

    @pl.when(outer | (core == 0))
    def _():
        signal(barrier, mate)

    @pl.when(outer)
    def _():
        pl.semaphore_wait(barrier, 2)

    @pl.when(outer & (core == 1))
    def _():
        signal(outer_in, beside_core + 1)

    vregs = state.shape[1]
    quarter = vregs // 4
    bits = vregs.bit_length() - 1
    width = vregs // owners
    full = 8 * n

    loads[0].wait()

    lane = lax.broadcasted_iota(jnp.int32, (8, 128), 1)
    sub = lax.broadcasted_iota(jnp.int32, (8, 128), 0)

    mid = sub_ref[1]
    lane_step = jnp.int32(1)
    for b in range(1, 7):
        lane_step = jnp.where(mid == b, 2**b, lane_step)
    top = 10 + bits - 1
    in_lane = (mid < 7) | (mid == top - 1)
    stride = jnp.int32(vregs // 8)
    for b in range(10, top - 1):
        stride = jnp.where(mid == b, 2 ** (b - 10), stride)
    stride = jnp.where(mid == 7, vregs // 4, stride)
    stride = jnp.where(mid == 9, vregs // 2, stride)
    fixed = mid == 8
    lane_on = jnp.where(in_lane, lane_step, 0)
    lane_hit = jnp.bitwise_and(lane, lane_on) != 0
    lane_keep = lane_hit | (jnp.where(in_lane, 0, 1) != jnp.bitwise_and(lane, 0))
    sub_on = jnp.where(fixed, 0, 2)
    sub_hit = jnp.bitwise_and(sub, sub_on) != 0
    sub_keep = sub_hit | (jnp.where(fixed, 1, 0) != jnp.bitwise_and(sub, 0))

    high4 = sub >= 4
    odd_sub = jnp.bitwise_and(sub, 1) != 0
    odd_lane = jnp.bitwise_and(lane, 1) != 0

    def swap(a, b, hit, keep, step, axis):
        size = (8, 128)[axis]
        back = size - step
        return (
            jnp.where(hit, pltpu.roll(b, step, axis), a),
            jnp.where(keep, b, pltpu.roll(a, back, axis)),
        )

    def spread(c, v):
        x = [state[c, v + quarter * k] for k in range(4)]
        x[0], x[2] = swap(x[0], x[2], high4, high4, 4, 0)
        x[1], x[3] = swap(x[1], x[3], high4, high4, 4, 0)
        for k in (0, 2):
            a, b = swap(x[k], x[k + 1], odd_lane, odd_lane, 1, 1)
            x[k], x[k + 1] = swap(a, b, odd_sub, odd_sub, 1, 0)
        return x

    def fresh(c, at):
        x = spread(c, lax.rem(at, quarter))
        for k in range(3):
            x[3] = jnp.where(at // quarter == k, x[k], x[3])
        return x[3]

    def first_pass(v, carry):
        for c in range(2):
            for k, value in enumerate(spread(c, v)):
                mixed[c, v + quarter * k] = value
        return carry

    pairs = width // 2
    send, recv = (send_a, send_b), (recv_a, recv_b)
    high_ref, low_ref = (high_a, high_b), (low_a, low_b)
    tiles = piece_tiles(width)
    def target(zone, k):
        return zone * chips + jnp.bitwise_xor(chip, chips - 1 - k)

    def pack(owner, read):
        for c in range(2):
            for p in range(pairs):
                u = owner * pairs + p
                low = jnp.bitwise_and(u, stride - 1)
                first = 2 * u - low
                a = read(c, first)
                b = read(c, first + stride)
                a, b = swap(a, b, lane_hit, lane_keep, lane_step, 1)
                a, b = swap(a, b, sub_hit, sub_keep, 2, 0)
                for w, value in enumerate((a, b)):
                    tile = 2 * p + w
                    piece = int(tile >= tiles[0])
                    column = (c * tiles[piece] + tile - piece * tiles[0]) * 128
                    send[piece][owner, :, column : column + 128] = value

    def pack_group(zone, start):
        def one(k, carry):
            pack(target(zone, k), lambda c, at: mixed[c, at])
            return carry

        lax.fori_loop(start, chips, one, 0, unroll=4 - start if chips >= 4 else 1)

    def send_group(zone, start, stop):
        for piece in range(2):
            def one(k, carry):
                owner = target(zone, k)
                device = 2 * owner + 1
                arrived = recv_sem.at[plane, piece]
                source, there = send[piece].at[owner], recv[piece].at[me]

                @pl.when(device != me)
                def _():
                    pltpu.make_async_remote_copy(
                        src_ref=source, dst_ref=there, send_sem=send_sem, recv_sem=arrived,
                        device_id=(device,), device_id_type=MESH,
                    ).start()

                @pl.when(device == me)
                def _():
                    pltpu.make_async_copy(source, there, arrived).start()

                return carry

            lax.fori_loop(start, stop, one, 0)

    for load in loads[1:]:
        load.wait()
    pack(target(across, 0), fresh)
    @pl.when(inner)
    def _():
        pl.semaphore_wait(barrier, owners // 2)

    @pl.when(outer)
    def _():
        pl.semaphore_wait(go.at[0], 1)

    @pl.when(outer & (core == 1))
    def _():
        signal(go.at[0], mate)

    send_group(across, 0, 1)

    @pl.when(inner & (core == 1))
    def _():
        pl.semaphore_wait(outer_in, 1)
        signal(go.at[0], beside_core + 1)

        def tell(k, carry):
            device = devs + 2 * k + 1

            @pl.when(device != me)
            def _():
                signal(column_in, device)

            return carry

        lax.fori_loop(0, owners // 2, tell, 0)

    lax.fori_loop(0, quarter, first_pass, 0, unroll=16)
    pack_group(far, 0)

    @pl.when(inner & (core == 1))
    def _():
        pl.semaphore_wait(column_in, owners // 2 - 1)
        signal(go.at[1], mate)
        signal(go.at[1], beside_core + 1)

    @pl.when(outer | (core == 0))
    def _():
        pl.semaphore_wait(go.at[1], 1)

    @pl.when(outer & (core == 1))
    def _():
        signal(go.at[1], mate)

    send_group(far, 0, chips)
    pack_group(beside, 0)
    send_group(beside, 0, chips)
    pack_group(across, 1)
    send_group(across, 1, chips)
    pack_group(plane, 0)
    send_group(plane, 0, chips)

    @pl.when(core == 0)
    def _():
        def tell(k, carry):
            signal(present, 2 * k + 1)
            return carry

        lax.fori_loop(0, owners, tell, 0)


    block = 8 * devs
    wide = max(block, 128)
    ratio = wide // block
    columns = full // 2

    def split(x):
        high = x.astype(jnp.bfloat16)
        return high, (x - high.astype(jnp.float32)).astype(jnp.bfloat16)

    def dot(x, y):
        return lax.dot_general(x, y, (((1,), (1,)), ((), ())), preferred_element_type=jnp.float32)

    def stacked(x):
        depth = x.shape[1] // 2
        return jnp.concatenate(
            [x, jnp.concatenate([x[:, depth:], -x[:, :depth]], axis=1)], axis=0
        )

    def arrival(s):
        second = jnp.where(outer, far, beside)
        third = jnp.where(outer, across, far)
        last = jnp.where(outer, beside, across)
        return jnp.where(
            s == 0, plane, jnp.where(s == 1, second, jnp.where(s == 2, third, last))
        )

    def gram(at, piece):
        zone = arrival(at)
        mine = pl.ds(zone * devs, devs)
        lines = pl.ds(pl.multiple_of(zone * block, block), block)
        came = recv[piece].at[mine]
        pltpu.make_async_copy(came, came, recv_sem.at[zone, piece]).wait()
        high, low = split(recv[piece][mine].reshape(block, 256 * tiles[piece]))
        high_ref[piece][lines] = high
        low_ref[piece][lines] = low
        left_h = stacked(high)
        both = dot(jnp.concatenate([left_h, stacked(low)], axis=0), high_ref[piece][...])
        result = both[: 2 * block] + (both[2 * block :] + dot(left_h, low_ref[piece][...]))
        start = lax.rem(zone * block, columns) // wide * wide
        for c in range(2):
            value = result[c * block : (c + 1) * block]
            here = slice(c * columns, (c + 1) * columns)
            for side in range(2):
                added = value[:, side * columns : (side + 1) * columns]
                part[mine, side, :, here] = part[mine, side, :, here] + added.reshape(
                    devs, 8, columns
                )
            if c == 1:
                value = -value
            if ratio > 1:
                slot = lax.rem(zone, ratio)
                value = jnp.concatenate(
                    [jnp.where(slot == r, value, 0.0) for r in range(ratio)], axis=0
                )
            turned_ref[c] = value.T.reshape(n, 8, wide)

        def mirror(e, carry):
            there = pl.ds(arrival(e) * devs, devs)
            for c in range(2):
                span = pl.ds(pl.multiple_of(c * columns + start, 128), wide)
                part[there, zone // 2, :, span] = (
                    part[there, zone // 2, :, span] + turned_ref[c, there]
                )
            return carry

        lax.fori_loop(0, at, mirror, 0)

    def send_rows(zone, slot, half=None, ready=None, first=0, last=devs):
        def one(k, carry):
            device = zone * devs + k
            if ready is not None:
                ready(device)
            if half is None:
                source, target_rows = part.at[device], rows.at[slot, chip]
            else:
                source, target_rows = part.at[device, half], rows.at[slot, chip, half]

            @pl.when(device != me)
            def _():
                pltpu.make_async_remote_copy(
                    src_ref=source, dst_ref=target_rows, send_sem=row_send,
                    recv_sem=row_recv.at[slot], device_id=(device,), device_id_type=MESH,
                ).start()

            @pl.when(device == me)
            def _():
                pltpu.make_async_copy(source, target_rows, row_recv.at[slot]).start()

            return carry

        lax.fori_loop(first, last, one, 0)

    def add_chain(device):
        part[device] = part[device] + chain[device]

    @pl.when(core == 1)
    def _():
        pl.semaphore_wait(present, owners)
        for ref in (*high_ref, *low_ref, part):
            ref[...] = jnp.zeros_like(ref)

        near = plane // 2

        def step(i, carry):
            crossed = outer & (i >= 4)
            at = jnp.where(crossed, 2 + lax.rem(i, 2), i // 2)
            piece = jnp.where(crossed, i // 2 - 2, lax.rem(i, 2))
            for p in range(2):
                pl.when(piece == p)(functools.partial(gram, at, p))

            @pl.when(inner & ((i == 4) | (i == 7)))
            def _():
                send_rows(beside, 1, jnp.where(i == 4, near, 1 - near))

            return carry

        lax.fori_loop(0, 2 * PLANES, step, 0)

        @pl.when(outer)
        def _():
            for i in range(4):
                mine = pl.ds((far, across)[i // 2] * devs + i % 2 * chips, chips)
                pltpu.make_async_remote_copy(
                    src_ref=part.at[mine], dst_ref=chain.at[mine], send_sem=row_send,
                    recv_sem=chain_sem.at[i], device_id=(beside * devs + 2 * chip + 1,),
                    device_id_type=MESH,
                ).start()
            send_rows(beside, 1)
            send_rows(plane, 0)

        @pl.when(inner)
        def _():
            def relay(i, carry):
                zone, first = jnp.where(i < 2, far, across), lax.rem(i, 2) * chips
                came = chain.at[pl.ds(zone * devs + first, chips)]
                pltpu.make_async_copy(came, came, chain_sem.at[i]).wait()
                send_rows(zone, 2, ready=add_chain, first=first, last=first + chips)
                return carry

            lax.fori_loop(0, 4, relay, 0)
            send_rows(plane, 0)

    for ref in send:
        rest = ref.at[pl.ds(0, owners - 1)]
        pltpu.make_async_copy(rest, rest, send_sem).wait()

    @pl.when(core == 0)
    def _():
        for ref in send:
            pltpu.make_async_copy(ref.at[0], ref.at[0], send_sem).wait()

    @pl.when(core == 1)
    def _():
        sent = part.at[pl.ds(0, n - 1)]
        pltpu.make_async_copy(sent, sent, row_send).wait()

    def gather(slot, total):
        came = rows.at[slot]
        pltpu.make_async_copy(came, came, row_recv.at[slot]).wait()
        for k in range(chips):
            total = total + rows[slot, k]
        return total

    total = lax.fori_loop(0, 3, gather, jnp.zeros((2, 8, full), jnp.float32)) * scale
    for side in range(2):
        for c in range(2):
            at = c * full + side * columns
            out_ref[:, at : at + columns] = total[side, :, c * columns : (c + 1) * columns]


def local(n, state_real, state_imag, subsystem):
    amps = state_real.shape[0]
    vregs = amps // 1024
    owners = n // 2
    width = vregs // owners
    full = 8 * n
    devs = n // PLANES
    wide = max(8 * devs, 128)
    depths = [256 * tiles for tiles in piece_tiles(width)]
    out = pl.pallas_call(
        functools.partial(exchange_kernel, n, 8.0 / amps),
        out_shape=pltpu.VMEM((8, 2 * full), jnp.float32),
        in_specs=[
            pl.BlockSpec(memory_space=pl.ANY),
            pl.BlockSpec(memory_space=pl.ANY),
            pl.BlockSpec(memory_space=pl.ANY),
        ],
        out_specs=pl.BlockSpec(memory_space=pltpu.VMEM),
        scratch_shapes=[
            pltpu.SMEM((3,), jnp.int32),
            pltpu.VMEM((2, vregs, 8, 128), jnp.float32),
            pltpu.VMEM((2, vregs, 8, 128), jnp.float32),
            *[pltpu.VMEM((owners, 8, depth), jnp.float32) for depth in depths],
            *[pltpu.VMEM((n, 8, depth), jnp.float32) for depth in depths],
            *[pltpu.VMEM((full, depth), jnp.bfloat16) for depth in depths],
            *[pltpu.VMEM((full, depth), jnp.bfloat16) for depth in depths],
            pltpu.VMEM((n, 2, 8, full), jnp.float32),
            pltpu.VMEM((2, n, 8, wide), jnp.float32),
            pltpu.VMEM((n, 2, 8, full), jnp.float32),
            pltpu.VMEM((3, devs // 2, 2, 8, full), jnp.float32),
            pltpu.SemaphoreType.DMA((3,)),
            pltpu.SemaphoreType.DMA,
            pltpu.SemaphoreType.DMA((PLANES, 2)),
            pltpu.SemaphoreType.DMA((4,)),
            pltpu.SemaphoreType.DMA,
            pltpu.SemaphoreType.DMA((3,)),
            pltpu.SemaphoreType.REGULAR,
            pltpu.SemaphoreType.REGULAR,
            pltpu.SemaphoreType.REGULAR,
            pltpu.SemaphoreType.REGULAR((2,)),
        ],
        compiler_params=pltpu.CompilerParams(
            collective_id=0, has_side_effects=True, vmem_limit_bytes=56 * 2**20
        ),
    )(subsystem, state_real.reshape(vregs, 8, 128), state_imag.reshape(vregs, 8, 128))
    return out[:, :full], out[:, full:]


def solution(mesh):
    return jax.shard_map(
        functools.partial(local, mesh.shape["dev"]),
        mesh=mesh,
        in_specs=(P("dev"), P("dev"), P()),
        out_specs=(P("dev", None), P("dev", None)),
        check_vma=False,
    )
```

```python
import functools

import jax
import jax.numpy as jnp
from jax import lax
from jax.experimental import pallas as pl
from jax.experimental.pallas import tpu as pltpu
from jax.sharding import PartitionSpec as P

MESH = pl.DeviceIdType.MESH
PLANES = 4


def piece_tiles(width):
    last = max(1, width // 4)
    return width - last, last


def exchange_kernel(n, scale, sub_hbm, re_hbm, im_hbm, out_ref, sub_ref, state, mixed, send_a,
                    send_b, recv_a, recv_b, high_a, high_b, low_a, low_b, part, turned_ref, chain, rows, load_sem, send_sem,
                    recv_sem, chain_sem, row_send, row_recv, present, outer_in, column_in, go):
    me = lax.axis_index("dev")
    loads = [
        pltpu.make_async_copy(sub_hbm, sub_ref, load_sem.at[2]),
        pltpu.make_async_copy(re_hbm, state.at[0], load_sem.at[0]),
        pltpu.make_async_copy(im_hbm, state.at[1], load_sem.at[1]),
    ]
    for load in loads:
        load.start()
    barrier = pltpu.get_barrier_semaphore()

    devs = n // PLANES
    chips = devs // 2
    owners = n // 2
    plane = me // devs
    chip = lax.rem(me, devs) // 2
    core = lax.rem(me, 2)
    low_half = plane < 2
    outer = (plane == 0) | (plane == PLANES - 1)
    inner = jnp.logical_not(outer)
    beside = jnp.bitwise_xor(plane, 1)
    far = jnp.where(low_half, 3, 0)
    across = jnp.where(low_half, 2, 1)

    mate = jnp.bitwise_xor(me, 1)

    def signal(sem, device):
        pl.semaphore_signal(sem, inc=1, device_id=(device,), device_id_type=MESH)

    beside_core = beside * devs + 2 * chip

    @pl.when(inner & (core == 1))
    def _():
        def greet(k, carry):
            device = devs + k

            @pl.when(device != me)
            def _():
                signal(barrier, device)

            return carry

        lax.fori_loop(0, 2 * devs, greet, 0)
        signal(barrier, beside_core)
        signal(barrier, beside_core + 1)

    @pl.when(outer | (core == 0))
    def _():
        signal(barrier, mate)

    @pl.when(outer)
    def _():
        pl.semaphore_wait(barrier, 2)

    @pl.when(outer & (core == 1))
    def _():
        signal(outer_in, beside_core + 1)

    vregs = state.shape[1]
    quarter = vregs // 4
    bits = vregs.bit_length() - 1
    width = vregs // owners
    full = 8 * n

    loads[0].wait()

    lane = lax.broadcasted_iota(jnp.int32, (8, 128), 1)
    sub = lax.broadcasted_iota(jnp.int32, (8, 128), 0)

    mid = sub_ref[1]
    lane_step = jnp.int32(1)
    for b in range(1, 7):
        lane_step = jnp.where(mid == b, 2**b, lane_step)
    top = 10 + bits - 1
    in_lane = (mid < 7) | (mid == top - 1)
    stride = jnp.int32(vregs // 8)
    for b in range(10, top - 1):
        stride = jnp.where(mid == b, 2 ** (b - 10), stride)
    stride = jnp.where(mid == 7, vregs // 4, stride)
    stride = jnp.where(mid == 9, vregs // 2, stride)
    fixed = mid == 8
    lane_on = jnp.where(in_lane, lane_step, 0)
    lane_hit = jnp.bitwise_and(lane, lane_on) != 0
    lane_keep = lane_hit | (jnp.where(in_lane, 0, 1) != jnp.bitwise_and(lane, 0))
    sub_on = jnp.where(fixed, 0, 2)
    sub_hit = jnp.bitwise_and(sub, sub_on) != 0
    sub_keep = sub_hit | (jnp.where(fixed, 1, 0) != jnp.bitwise_and(sub, 0))

    high4 = sub >= 4
    odd_sub = jnp.bitwise_and(sub, 1) != 0
    odd_lane = jnp.bitwise_and(lane, 1) != 0

    def swap(a, b, hit, keep, step, axis):
        size = (8, 128)[axis]
        back = size - step
        return (
            jnp.where(hit, pltpu.roll(b, step, axis), a),
            jnp.where(keep, b, pltpu.roll(a, back, axis)),
        )

    def spread(c, v):
        x = [state[c, v + quarter * k] for k in range(4)]
        x[0], x[2] = swap(x[0], x[2], high4, high4, 4, 0)
        x[1], x[3] = swap(x[1], x[3], high4, high4, 4, 0)
        for k in (0, 2):
            a, b = swap(x[k], x[k + 1], odd_lane, odd_lane, 1, 1)
            x[k], x[k + 1] = swap(a, b, odd_sub, odd_sub, 1, 0)
        return x

    def fresh(c, at):
        x = spread(c, lax.rem(at, quarter))
        for k in range(3):
            x[3] = jnp.where(at // quarter == k, x[k], x[3])
        return x[3]

    def first_pass(v, carry):
        for c in range(2):
            for k, value in enumerate(spread(c, v)):
                mixed[c, v + quarter * k] = value
        return carry

    pairs = width // 2
    send, recv = (send_a, send_b), (recv_a, recv_b)
    high_ref, low_ref = (high_a, high_b), (low_a, low_b)
    tiles = piece_tiles(width)
    def target(zone, k):
        return zone * chips + jnp.bitwise_xor(chip, chips - 1 - k)

    def pack(owner, read):
        for c in range(2):
            for p in range(pairs):
                u = owner * pairs + p
                low = jnp.bitwise_and(u, stride - 1)
                first = 2 * u - low
                a = read(c, first)
                b = read(c, first + stride)
                a, b = swap(a, b, lane_hit, lane_keep, lane_step, 1)
                a, b = swap(a, b, sub_hit, sub_keep, 2, 0)
                for w, value in enumerate((a, b)):
                    tile = 2 * p + w
                    piece = int(tile >= tiles[0])
                    column = (c * tiles[piece] + tile - piece * tiles[0]) * 128
                    send[piece][owner, :, column : column + 128] = value

    def pack_group(zone, start):
        def one(k, carry):
            pack(target(zone, k), lambda c, at: mixed[c, at])
            return carry

        lax.fori_loop(start, chips, one, 0, unroll=4 - start if chips >= 4 else 1)

    def send_group(zone, start, stop):
        for piece in range(2):
            def one(k, carry):
                owner = target(zone, k)
                device = 2 * owner + 1
                arrived = recv_sem.at[plane, piece]
                source, there = send[piece].at[owner], recv[piece].at[me]

                @pl.when(device != me)
                def _():
                    pltpu.make_async_remote_copy(
                        src_ref=source, dst_ref=there, send_sem=send_sem, recv_sem=arrived,
                        device_id=(device,), device_id_type=MESH,
                    ).start()

                @pl.when(device == me)
                def _():
                    pltpu.make_async_copy(source, there, arrived).start()

                return carry

            lax.fori_loop(start, stop, one, 0)

    for load in loads[1:]:
        load.wait()
    pack(target(across, 0), fresh)
    @pl.when(inner)
    def _():
        pl.semaphore_wait(barrier, owners // 2)

    @pl.when(outer)
    def _():
        pl.semaphore_wait(go.at[0], 1)

    @pl.when(outer & (core == 1))
    def _():
        signal(go.at[0], mate)

    send_group(across, 0, 1)

    @pl.when(inner & (core == 1))
    def _():
        pl.semaphore_wait(outer_in, 1)
        signal(go.at[0], beside_core + 1)

        def tell(k, carry):
            device = devs + 2 * k + 1

            @pl.when(device != me)
            def _():
                signal(column_in, device)

            return carry

        lax.fori_loop(0, owners // 2, tell, 0)

    lax.fori_loop(0, quarter, first_pass, 0, unroll=16)
    pack_group(far, 0)

    @pl.when(inner & (core == 1))
    def _():
        pl.semaphore_wait(column_in, owners // 2 - 1)
        signal(go.at[1], mate)
        signal(go.at[1], beside_core + 1)

    @pl.when(outer | (core == 0))
    def _():
        pl.semaphore_wait(go.at[1], 1)

    @pl.when(outer & (core == 1))
    def _():
        signal(go.at[1], mate)

    send_group(far, 0, chips)
    pack_group(beside, 0)
    send_group(beside, 0, chips)
    pack_group(across, 1)
    send_group(across, 1, chips)
    pack_group(plane, 0)
    send_group(plane, 0, chips)

    @pl.when(core == 0)
    def _():
        def tell(k, carry):
            signal(present, 2 * k + 1)
            return carry

        lax.fori_loop(0, owners, tell, 0)


    block = 8 * devs
    wide = max(block, 128)
    ratio = wide // block
    columns = full // 2

    def split(x):
        high = x.astype(jnp.bfloat16)
        return high, (x - high.astype(jnp.float32)).astype(jnp.bfloat16)

    def dot(x, y):
        return lax.dot_general(x, y, (((1,), (1,)), ((), ())), preferred_element_type=jnp.float32)

    def stacked(x):
        depth = x.shape[1] // 2
        return jnp.concatenate(
            [x, jnp.concatenate([x[:, depth:], -x[:, :depth]], axis=1)], axis=0
        )

    def arrival(s):
        second = jnp.where(outer, far, beside)
        third = jnp.where(outer, across, far)
        last = jnp.where(outer, beside, across)
        return jnp.where(
            s == 0, plane, jnp.where(s == 1, second, jnp.where(s == 2, third, last))
        )

    def gram(at, piece):
        zone = arrival(at)
        mine = pl.ds(zone * devs, devs)
        lines = pl.ds(pl.multiple_of(zone * block, block), block)
        came = recv[piece].at[mine]
        pltpu.make_async_copy(came, came, recv_sem.at[zone, piece]).wait()
        high, low = split(recv[piece][mine].reshape(block, 256 * tiles[piece]))
        high_ref[piece][lines] = high
        low_ref[piece][lines] = low
        left_h = stacked(high)
        both = dot(jnp.concatenate([left_h, stacked(low)], axis=0), high_ref[piece][...])
        result = both[: 2 * block] + (both[2 * block :] + dot(left_h, low_ref[piece][...]))
        start = lax.rem(zone * block, columns) // wide * wide
        for c in range(2):
            value = result[c * block : (c + 1) * block]
            here = slice(c * columns, (c + 1) * columns)
            for side in range(2):
                added = value[:, side * columns : (side + 1) * columns]
                part[mine, side, :, here] = part[mine, side, :, here] + added.reshape(
                    devs, 8, columns
                )
            if c == 1:
                value = -value
            if ratio > 1:
                slot = lax.rem(zone, ratio)
                value = jnp.concatenate(
                    [jnp.where(slot == r, value, 0.0) for r in range(ratio)], axis=0
                )
            turned_ref[c] = value.T.reshape(n, 8, wide)

        def mirror(e, carry):
            there = pl.ds(arrival(e) * devs, devs)
            for c in range(2):
                span = pl.ds(pl.multiple_of(c * columns + start, 128), wide)
                part[there, zone // 2, :, span] = (
                    part[there, zone // 2, :, span] + turned_ref[c, there]
                )
            return carry

        lax.fori_loop(0, at, mirror, 0)

    def send_rows(zone, slot, half=None, ready=None, first=0, last=devs):
        def one(k, carry):
            device = zone * devs + k
            if ready is not None:
                ready(device)
            if half is None:
                source, target_rows = part.at[device], rows.at[slot, chip]
            else:
                source, target_rows = part.at[device, half], rows.at[slot, chip, half]

            @pl.when(device != me)
            def _():
                pltpu.make_async_remote_copy(
                    src_ref=source, dst_ref=target_rows, send_sem=row_send,
                    recv_sem=row_recv.at[slot], device_id=(device,), device_id_type=MESH,
                ).start()

            @pl.when(device == me)
            def _():
                pltpu.make_async_copy(source, target_rows, row_recv.at[slot]).start()

            return carry

        lax.fori_loop(first, last, one, 0)

    def add_chain(device):
        part[device] = part[device] + chain[device]

    @pl.when(core == 1)
    def _():
        pl.semaphore_wait(present, owners)
        for ref in (*high_ref, *low_ref, part):
            ref[...] = jnp.zeros_like(ref)

        near = plane // 2

        def step(i, carry):
            crossed = outer & (i >= 4)
            at = jnp.where(crossed, 2 + lax.rem(i, 2), i // 2)
            piece = jnp.where(crossed, i // 2 - 2, lax.rem(i, 2))
            for p in range(2):
                pl.when(piece == p)(functools.partial(gram, at, p))

            @pl.when(inner & ((i == 3) | (i == 7)))
            def _():
                send_rows(beside, 1, jnp.where(i == 3, near, 1 - near))

            return carry

        lax.fori_loop(0, 2 * PLANES, step, 0)

        @pl.when(outer)
        def _():
            for i in range(4):
                mine = pl.ds((far, across)[i // 2] * devs + i % 2 * chips, chips)
                pltpu.make_async_remote_copy(
                    src_ref=part.at[mine], dst_ref=chain.at[mine], send_sem=row_send,
                    recv_sem=chain_sem.at[i], device_id=(beside * devs + 2 * chip + 1,),
                    device_id_type=MESH,
                ).start()
            send_rows(beside, 1)
            send_rows(plane, 0)

        @pl.when(inner)
        def _():
            def relay(i, carry):
                zone, first = jnp.where(i < 2, far, across), lax.rem(i, 2) * chips
                came = chain.at[pl.ds(zone * devs + first, chips)]
                pltpu.make_async_copy(came, came, chain_sem.at[i]).wait()
                send_rows(zone, 2, ready=add_chain, first=first, last=first + chips)
                return carry

            lax.fori_loop(0, 4, relay, 0)
            send_rows(plane, 0)

    for ref in send:
        rest = ref.at[pl.ds(0, owners - 1)]
        pltpu.make_async_copy(rest, rest, send_sem).wait()

    @pl.when(core == 0)
    def _():
        for ref in send:
            pltpu.make_async_copy(ref.at[0], ref.at[0], send_sem).wait()

    @pl.when(core == 1)
    def _():
        sent = part.at[pl.ds(0, n - 1)]
        pltpu.make_async_copy(sent, sent, row_send).wait()

    def gather(slot, total):
        came = rows.at[slot]
        pltpu.make_async_copy(came, came, row_recv.at[slot]).wait()
        for k in range(chips):
            total = total + rows[slot, k]
        return total

    total = lax.fori_loop(0, 3, gather, jnp.zeros((2, 8, full), jnp.float32)) * scale
    for side in range(2):
        for c in range(2):
            at = c * full + side * columns
            out_ref[:, at : at + columns] = total[side, :, c * columns : (c + 1) * columns]


def local(n, state_real, state_imag, subsystem):
    amps = state_real.shape[0]
    vregs = amps // 1024
    owners = n // 2
    width = vregs // owners
    full = 8 * n
    devs = n // PLANES
    wide = max(8 * devs, 128)
    depths = [256 * tiles for tiles in piece_tiles(width)]
    out = pl.pallas_call(
        functools.partial(exchange_kernel, n, 8.0 / amps),
        out_shape=pltpu.VMEM((8, 2 * full), jnp.float32),
        in_specs=[
            pl.BlockSpec(memory_space=pl.ANY),
            pl.BlockSpec(memory_space=pl.ANY),
            pl.BlockSpec(memory_space=pl.ANY),
        ],
        out_specs=pl.BlockSpec(memory_space=pltpu.VMEM),
        scratch_shapes=[
            pltpu.SMEM((3,), jnp.int32),
            pltpu.VMEM((2, vregs, 8, 128), jnp.float32),
            pltpu.VMEM((2, vregs, 8, 128), jnp.float32),
            *[pltpu.VMEM((owners, 8, depth), jnp.float32) for depth in depths],
            *[pltpu.VMEM((n, 8, depth), jnp.float32) for depth in depths],
            *[pltpu.VMEM((full, depth), jnp.bfloat16) for depth in depths],
            *[pltpu.VMEM((full, depth), jnp.bfloat16) for depth in depths],
            pltpu.VMEM((n, 2, 8, full), jnp.float32),
            pltpu.VMEM((2, n, 8, wide), jnp.float32),
            pltpu.VMEM((n, 2, 8, full), jnp.float32),
            pltpu.VMEM((3, devs // 2, 2, 8, full), jnp.float32),
            pltpu.SemaphoreType.DMA((3,)),
            pltpu.SemaphoreType.DMA,
            pltpu.SemaphoreType.DMA((PLANES, 2)),
            pltpu.SemaphoreType.DMA((4,)),
            pltpu.SemaphoreType.DMA,
            pltpu.SemaphoreType.DMA((3,)),
            pltpu.SemaphoreType.REGULAR,
            pltpu.SemaphoreType.REGULAR,
            pltpu.SemaphoreType.REGULAR,
            pltpu.SemaphoreType.REGULAR((2,)),
        ],
        compiler_params=pltpu.CompilerParams(
            collective_id=0, has_side_effects=True, vmem_limit_bytes=56 * 2**20
        ),
    )(subsystem, state_real.reshape(vregs, 8, 128), state_imag.reshape(vregs, 8, 128))
    return out[:, :full], out[:, full:]


def solution(mesh):
    return jax.shard_map(
        functools.partial(local, mesh.shape["dev"]),
        mesh=mesh,
        in_specs=(P("dev"), P("dev"), P()),
        out_specs=(P("dev", None), P("dev", None)),
        check_vma=False,
    )
```
